512 devices in a mesh: gx: 8 (over x, core), gy: 8 (over y), gz: 8 (over z).
Axes of the slice: x: 4, y: 8, z: 8, core: 2. Of those that a mesh axis runs over, the one named last changes fastest.
Arguments:
- warped_image: float32 [512, 512, 1024], P('gx', 'gy', 'gz'), may hold values from -6 to 6
- fixed_image: float32 [512, 512, 1024], P('gx', 'gy', 'gz'), may hold values from -6 to 6
- fine_control: float32 [3, 64, 64, 128], P(None, 'gx', 'gy', 'gz'), may hold values from -6 to 6
- coarse_control: float32 [3, 16, 16, 32], replicated, may hold values from -6 to 6
Outputs:
- fine_gradient: float32 [3, 64, 64, 128], P(None, 'gx', 'gy', 'gz')
- coarse_gradient: float32 [3, 16, 16, 32], replicated
The draws below stay inside these ranges and needn't reach their ends.
All inputs are finite; a program needn't handle non-finite values.
Results may differ from the reference program's by a relative error of at most 0.0003.
Values sent between devices are 32-bit elements; how exact they have to be, the bound alone decides.
No kernel may reach another device: no remote copies, remote signals or barrier semaphores. Data moves between devices by JAX's collectives and lax.ppermute only.
A program may use at most 64 MiB of HBM per device.

```python
import jax
import jax.numpy as jnp
from jax import lax

SPF = 8
SPC = 32
NX = 512
NY = 512
NZ = 1024
FX = 64
FY = 64
FZ = 128
KX = 16
KY = 16
KZ = 32


def levels(key, shape, shards, low, largest):
    def one(position, shards_of):
        draws = jax.random.uniform(jax.random.fold_in(jax.random.fold_in(key, 6), position), (shards_of,), jnp.float32, low / len(shards), largest / len(shards))
        return jnp.repeat(jnp.exp(draws), shape[position] // shards_of).reshape((-1,) + (1,) * (len(shape) - position - 1))

    gain = one(*shards[0])
    for cut in shards[1:]:
        gain = gain * one(*cut)
    return gain


def scatter_about(rng, extent, deviation, most, cuts=(), kind=jnp.bfloat16):
    entries = deviation * jax.random.normal(rng, extent, jnp.float32)
    if cuts:
        entries = entries * levels(rng, extent, cuts, -0.22, 0.18)
    return jnp.clip(entries, -most, most).astype(kind)


def setup_inputs(seed: int = 0) -> dict:
    arg_keys = jax.random.split(jax.random.key(seed), 5)
    return {
        "warped_image": scatter_about(arg_keys[0], (NX, NY, NZ), 1.0, 6.0, ((0, 8), (1, 8), (2, 8)), jnp.float32),
        "fixed_image": scatter_about(arg_keys[1], (NX, NY, NZ), 1.0, 6.0, ((0, 8), (1, 8), (2, 8)), jnp.float32),
        "fine_control": scatter_about(arg_keys[2], (3, FX, FY, FZ), 1.0, 6.0, ((1, 8), (2, 8), (3, 8)), jnp.float32),
        "coarse_control": scatter_about(arg_keys[3], (3, KX, KY, KZ), 1.0, 6.0, (), jnp.float32),
    }


bend_factor = 0.01
highest = lax.Precision.HIGHEST


def spline(values):
    magnitude = jnp.abs(values)
    inner = 2.0 / 3.0 - magnitude * magnitude + 0.5 * magnitude * magnitude * magnitude
    remain = 2.0 - magnitude
    outer = remain * remain * remain / 6.0
    return jnp.where(magnitude < 1.0, inner, jnp.where(magnitude < 2.0, outer, 0.0 * magnitude))


def basis_matrix(voxels, points, spacing, voxel_start, point_start):
    voxel = (jnp.arange(voxels, dtype=jnp.int32) + voxel_start).astype(jnp.float32) + 0.5
    centre = (jnp.arange(points, dtype=jnp.int32) + point_start).astype(jnp.float32) * spacing + 0.5 * spacing
    return spline((voxel[:, None] - centre[None, :]) / spacing)


def slope(padded, axis):
    rank = padded.ndim
    count = padded.shape[axis] - 4

    def shifted(offset):
        piece = lax.slice_in_dim(padded, offset, offset + count, axis=axis)
        for other in range(rank - 3, rank):
            if other != axis:
                piece = lax.slice_in_dim(piece, 2, piece.shape[other] - 2, axis=other)
        return piece

    return (shifted(0) - 8.0 * shifted(1) + 8.0 * shifted(3) - shifted(4)) / 12.0


def stencil(padded):
    centre = padded[:, 1:-1, 1:-1, 1:-1]
    total = padded[:, 2:, 1:-1, 1:-1] + padded[:, :-2, 1:-1, 1:-1]
    total = total + padded[:, 1:-1, 2:, 1:-1] + padded[:, 1:-1, :-2, 1:-1]
    total = total + padded[:, 1:-1, 1:-1, 2:] + padded[:, 1:-1, 1:-1, :-2]
    return total - 6.0 * centre


def laplace(field):
    return stencil(jnp.pad(field, ((0, 0), (1, 1), (1, 1), (1, 1))))


def project_blocks(force, along_x, along_y, along_z):
    section = jnp.einsum("axyz,zr->axyr", force, along_z, precision=highest)
    section = jnp.einsum("axyr,yq->axqr", section, along_y, precision=highest)
    return jnp.einsum("axqr,xp->apqr", section, along_x, precision=highest)


def reference(warped_image, fixed_image, fine_control, coarse_control):
    summed = jnp.pad(warped_image + fixed_image, 2)
    difference = warped_image - fixed_image
    fine_x = basis_matrix(NX, FX, SPF, 0, 0)
    fine_y = basis_matrix(NY, FY, SPF, 0, 0)
    fine_z = basis_matrix(NZ, FZ, SPF, 0, 0)
    coarse_x = basis_matrix(NX, KX, SPC, 0, 0)
    coarse_y = basis_matrix(NY, KY, SPC, 0, 0)
    coarse_z = basis_matrix(NZ, KZ, SPC, 0, 0)
    block_rows = 16

    def block(carry, start):
        fine_sum, coarse_sum = carry
        slab = lax.dynamic_slice_in_dim(summed, start, block_rows + 4, 0)
        slopes = jnp.stack([slope(slab, 0), slope(slab, 1), slope(slab, 2)]) * 0.5
        local = lax.dynamic_slice_in_dim(difference, start, block_rows, 0)
        force = slopes * local[None]
        fine_rows = lax.dynamic_slice_in_dim(fine_x, start, block_rows, 0)
        coarse_rows = lax.dynamic_slice_in_dim(coarse_x, start, block_rows, 0)
        fine_sum = fine_sum + project_blocks(force, fine_rows, fine_y, fine_z)
        coarse_sum = coarse_sum + project_blocks(force, coarse_rows, coarse_y, coarse_z)
        return (fine_sum, coarse_sum), None

    starts = jnp.arange(NX // block_rows, dtype=jnp.int32) * block_rows
    initial = (jnp.zeros((3, FX, FY, FZ), jnp.float32), jnp.zeros((3, KX, KY, KZ), jnp.float32))
    (fine_sum, coarse_sum), _ = lax.scan(block, initial, starts)
    fine_gradient = fine_sum * (SPF ** -1.5) + bend_factor * laplace(laplace(fine_control))
    coarse_gradient = coarse_sum * (SPC ** -1.5) + bend_factor * laplace(laplace(coarse_control))
    return fine_gradient, coarse_gradient
```

```python
import functools

import jax
import jax.numpy as jnp
import numpy as np
from jax import lax
from jax.experimental import pallas as pl
from jax.experimental.pallas import tpu as pltpu
from jax.sharding import PartitionSpec as P

SPF = 8
SPC = 32
BEND = 0.01
f32 = jnp.float32
bf16 = jnp.bfloat16
VMEM = pltpu.VMEM


def spline(t):
    t = np.abs(t)
    inner = 2.0 / 3.0 - t * t + 0.5 * t**3
    outer = (2.0 - t) ** 3 / 6.0
    return np.where(t < 1.0, inner, np.where(t < 2.0, outer, 0.0))


def weights(voxels, points, spacing):
    centre = (np.arange(points) - 2) * spacing + spacing / 2
    return spline((np.asarray(voxels)[:, None] + 0.5 - centre[None, :]) / spacing)


def halves(matrix):
    matrix = np.asarray(matrix, np.float32)
    high = matrix.astype(bf16)
    return high, (matrix - high.astype(np.float32)).astype(bf16)


def split(values):
    high = values.astype(bf16)
    return high, (values - high.astype(f32)).astype(bf16)


def mm(a, b):
    return jnp.dot(a, b, preferred_element_type=f32)


def mm3(values, high, low):
    a, b = split(values)
    return mm(a, high) + mm(b, high) + mm(a, low)


def lanes(shape):
    return lax.broadcasted_iota(jnp.int32, shape, len(shape) - 1)


def rows_of(shape):
    return lax.broadcasted_iota(jnp.int32, shape, len(shape) - 2)


def rolled(values, shift):
    shift %= values.shape[-1]
    return values if shift == 0 else pltpu.roll(values, shift, values.ndim - 1)


def whole(n):
    return [pl.BlockSpec(memory_space=VMEM)] * n


STEP = 16


def faces_kernel(w_ref, f_ref, xf_ref, yf_ref, zf_ref):
    g = pl.program_id(0)
    lane = lanes((64, 128))
    packed_s = jnp.zeros((64, 128), f32)
    packed_d = jnp.zeros((64, 128), f32)
    for i in range(STEP):
        w = w_ref[i]
        f = f_ref[i]
        s = w + f
        d = w - f
        yf_ref[i, 0:2, :] = s[62:64]
        yf_ref[i, 2:4, :] = d[62:64]
        here = (lane >= 4 * i) & (lane < 4 * i + 4)
        packed_s = jnp.where(here, rolled(s, 4 * i + 2), packed_s)
        packed_d = jnp.where(here, rolled(d, 4 * i + 2), packed_d)
        if i >= STEP - 2:

            @pl.when(g == 3)
            def _():
                xf_ref[i - (STEP - 2)] = s
                xf_ref[2 + i - (STEP - 2)] = d

    half = g // 2

    @pl.when(g % 2 == 0)
    def _():
        zf_ref[half] = packed_s
        zf_ref[2 + half] = packed_d

    @pl.when(g % 2 == 1)
    def _():
        zf_ref[half] = jnp.where(lane < 64, zf_ref[half], rolled(packed_s, 64))
        zf_ref[2 + half] = jnp.where(lane < 64, zf_ref[2 + half], rolled(packed_d, 64))


def faces(w, f):
    block = pl.BlockSpec((STEP, 64, 128), lambda g: (g, 0, 0))
    fixed = pl.BlockSpec((4, 64, 128), lambda g: (0, 0, 0))
    return pl.pallas_call(
        faces_kernel,
        grid=(64 // STEP,),
        in_specs=[block, block],
        out_specs=[fixed, pl.BlockSpec((STEP, 4, 128), lambda g: (g, 0, 0)), fixed],
        out_shape=[
            jax.ShapeDtypeStruct((4, 64, 128), f32),
            jax.ShapeDtypeStruct((64, 4, 128), f32),
            jax.ShapeDtypeStruct((4, 64, 128), f32),
        ],
        name="faces",
    )(w, f)


def bend_kernel(sizes, c_ref, k_ref, bf_ref, bk_ref, u_ref, a_ref, b_ref):
    nx, ny, nz = sizes
    ix, iy, iz = (lax.axis_index(n) for n in ("gx", "gy", "gz"))
    u_ref[...] = jnp.zeros_like(u_ref)
    for a in range(3):
        for p in range(8):
            at = 20 * (p + 2) + 2
            u_ref[a * 16 + 2 : a * 16 + 10, at : at + 16] = c_ref[a, p]
    lane = lanes((48, 256))
    row = rows_of((48, 256)) % 16
    gp = lane // 20 - 2 + 8 * ix
    gr = lane % 20 - 2 + 16 * iz
    gq = row - 2 + 8 * iy
    inside = (gp >= 0) & (gp < 8 * nx) & (gq >= 0) & (gq < 8 * ny) & (gr >= 0) & (gr < 16 * nz)

    def around(u):
        total = pltpu.roll(u, 1, 0) + pltpu.roll(u, 47, 0)
        for shift in (1, 255, 20, 236):
            total = total + pltpu.roll(u, shift, 1)
        return total - 6.0 * u

    u = around(u_ref[...])
    u = around(jnp.where(inside, u, 0.0)) * BEND
    keep = lanes((48, 128)) < 120
    bf_ref[:, 0:128] = jnp.where(keep, u[:, 0:128], 0.0)
    bf_ref[:, 128:256] = jnp.where(keep, pltpu.roll(u, 136, 1)[:, 0:128], 0.0)

    kx, ky, kz = 2 * nx, 2 * ny, 4 * nz
    a_ref[...] = jnp.zeros_like(a_ref)
    b_ref[...] = jnp.zeros_like(b_ref)
    for a in range(3):
        for p in range(kx):
            a_ref[a, p + 1, 8 : 8 + ky, 0:kz] = k_ref[a, p]
    grid = lanes((ky, 128)) < kz

    def star(ref, a, p):
        mid = ref[a, p + 1, 8 : 8 + ky, :]
        total = ref[a, p, 8 : 8 + ky, :] + ref[a, p + 2, 8 : 8 + ky, :]
        total = total + ref[a, p + 1, 7 : 7 + ky, :] + ref[a, p + 1, 9 : 9 + ky, :]
        total = total + rolled(mid, 1) + rolled(mid, 127)
        return total - 6.0 * mid

    for a in range(3):
        for p in range(kx):
            b_ref[a, p + 1, 8 : 8 + ky, :] = jnp.where(grid, star(a_ref, a, p), 0.0)
    for a in range(3):
        for p in range(kx):
            bk_ref[a, p] = (star(b_ref, a, p) * BEND)[:, 0:kz]


def bend(sizes, control, coarse):
    nx, ny, nz = sizes
    grid = (3, 2 * nx + 2, 2 * ny + 16, 128)
    return pl.pallas_call(
        functools.partial(bend_kernel, sizes),
        in_specs=whole(2),
        out_specs=whole(2),
        out_shape=[
            jax.ShapeDtypeStruct((48, 256), f32),
            jax.ShapeDtypeStruct(coarse.shape, f32),
        ],
        scratch_shapes=[VMEM((48, 256), f32), VMEM(grid, f32), VMEM(grid, f32)],
        cost_estimate=pl.CostEstimate(flops=4000000, bytes_accessed=1000000, transcendentals=0),
        name="bend",
    )(control, coarse)


@functools.cache
def tables():
    own = np.arange(64)
    cross = np.arange(-2, 2)
    wy = np.zeros((24, 64))
    wy[0:12] = weights(own, 12, SPF).T
    wy[16:22] = weights(own, 6, SPC).T
    high, low = halves(wy)
    left = np.concatenate(
        [np.concatenate([high, high], 1), np.concatenate([low, np.zeros_like(low)], 1)], 0
    )
    wc = np.zeros((8, 8, 128), np.float32)
    for j in range(4):
        wc[j, :, :] = weights(cross, 12, SPF)[j, 0:8, None]
        wc[4 + j, 0:6, :] = weights(cross, 6, SPC)[j, :, None]
    fine_scale = SPF**-1.5 / 24.0
    coarse_scale = SPC**-1.5 / 24.0
    wz = np.zeros((2, 128, 128))
    wz[0, :, 0:20] = weights(np.arange(128), 20, SPF) * fine_scale
    wz[1, :, 0:8] = weights(np.arange(128), 8, SPC) * coarse_scale
    wz_high, wz_low = halves(wz)
    m = np.zeros((2, 128, 384))
    fx, cx = weights(own, 12, SPF), weights(own, 6, SPC)
    fz = weights(cross, 20, SPF) * fine_scale
    cz = weights(cross, 8, SPC) * coarse_scale
    for x in range(64):
        for j in range(4):
            line = m[x // 32, 4 * (x % 32) + j]
            for p in range(12):
                at = 128 * (p // 6) + 20 * (p % 6)
                line[at : at + 20] = fx[x, p] * fz[j]
            for p in range(6):
                at = 256 + 80 + 8 * p
                line[at : at + 8] = cx[x, p] * cz[j]
    m_high, m_low = halves(m)
    coarse_x = weights(own, 6, SPC).astype(np.float32).reshape(-1)
    return left, wc, wz_high, wz_low, m_high, m_low, coarse_x


def project_kernel(
    w_ref, f_ref, xr_ref, yr_ref, zr_ref, zo_ref, bf_ref, left_ref, wc_ref, wzh_ref, wzl_ref, mh_ref, ml_ref, cx_ref,
    chunk_ref, fine_ref, s_ref, tf_ref, tc_ref, af_ref, ac_ref,
):
    n = chunk_ref.shape[0]
    fx = weights(np.arange(8), 5, SPF)
    edge_f = weights(np.arange(-2, 0), 4, SPF)
    edge_c = weights(np.arange(-2, 0), 4, SPC)

    s_ref[:, 0:8, :] = jnp.zeros((68, 8, 128), f32)
    s_ref[:, 72:80, :] = jnp.zeros((68, 8, 128), f32)
    s_ref[66:68, 8:72, :] = jnp.zeros((2, 64, 128), f32)
    s_ref[0:2, 8:72, :] = xr_ref[0:2]

    def add(x, carry):
        s_ref[x + 2, 8:72, :] = w_ref[x] + f_ref[x]
        return carry

    lax.fori_loop(0, 64, add, 0, unroll=8)

    left = left_ref[...]
    lane = lanes((64, 128))

    def along_y(force):
        high, low = split(force)
        both = mm(left, jnp.concatenate([high, low], 0))
        return both[0:24] + both[24:48]

    def layer(x, carry):
        s = s_ref[x + 2, 8:72, :]
        d = w_ref[x] - f_ref[x]
        below, above = s_ref[x + 1, 8:72, :], s_ref[x + 3, 8:72, :]
        f0 = (s_ref[x, 8:72, :] - s_ref[x + 4, 8:72, :]) + 8.0 * (above - below)
        f1 = (s_ref[x + 2, 6:70, :] - s_ref[x + 2, 10:74, :]) + 8.0 * (
            s_ref[x + 2, 9:73, :] - s_ref[x + 2, 7:71, :]
        )
        f2 = jnp.where(lane >= 2, rolled(s, 2), 0.0) - jnp.where(lane < 126, rolled(s, 126), 0.0)
        f2 = f2 + 8.0 * (
            jnp.where(lane < 127, rolled(s, 127), 0.0) - jnp.where(lane >= 1, rolled(s, 1), 0.0)
        )
        t = along_y(jnp.concatenate([f0 * d, f1 * d, f2 * d], 1))
        s0, s1 = s_ref[x + 2, 8:9, :], s_ref[x + 2, 9:10, :]
        d0, d1 = d[0:1], d[1:2]
        sm2, sm1 = yr_ref[x, 0:1, :], yr_ref[x, 1:2, :]
        dm2, dm1 = yr_ref[x, 2:3, :], yr_ref[x, 3:4, :]
        products = (-s0 * dm2, (8.0 * s0 - s1) * dm1, (sm2 - 8.0 * sm1) * d0, sm1 * d1)
        fine = t[0:8, 128:256]
        coarse = t[16:24, 128:256]
        for j in range(4):
            spread = jnp.broadcast_to(products[j], (8, 128))
            fine = fine + wc_ref[j] * spread
            coarse = coarse + wc_ref[4 + j] * spread
        for a in range(3):
            cols = slice(128 * a, 128 * a + 128)
            tf_ref[x, 16 * a : 16 * a + 8, :] = fine if a == 1 else t[0:8, cols]
            tf_ref[x, 16 * a + 8 : 16 * a + 16, :] = t[8:16, cols]
            tc_ref[x, 8 * a : 8 * a + 8, :] = coarse if a == 1 else t[16:24, cols]
        return carry

    lax.fori_loop(0, 64, layer, 0, unroll=2)

    af_ref[...] = jnp.zeros_like(af_ref)
    ac_ref[...] = jnp.zeros_like(ac_ref)

    s0, s1 = s_ref[2, 8:72, :], s_ref[3, 8:72, :]
    edge = along_y(jnp.concatenate([-s0 * xr_ref[2], (8.0 * s0 - s1) * xr_ref[3]], 1))
    for k in range(4):
        af_ref[k, 0:16, :] = float(edge_f[0, k]) * edge[0:16, 0:128] + float(edge_f[1, k]) * edge[0:16, 128:256]
        ac_ref[k, 0:8, :] = float(edge_c[0, k]) * edge[16:24, 0:128] + float(edge_c[1, k]) * edge[16:24, 128:256]

    def block(b, carry):
        for k in range(5):
            total = None
            for r in range(8):
                weight = float(fx[r, k])
                if weight == 0.0:
                    continue
                term = weight * tf_ref[8 * b + r]
                total = term if total is None else total + term
            af_ref[b + k] += total
        for k in range(6):
            total = None
            for r in range(8):
                term = cx_ref[(8 * b + r) * 6 + k] * tc_ref[8 * b + r]
                total = term if total is None else total + term
            ac_ref[k] += total
        return carry

    lax.fori_loop(0, 8, block, 0)

    zf = mm3(af_ref[...].reshape(576, 128), wzh_ref[0], wzl_ref[0])
    zc = mm3(ac_ref[...].reshape(144, 128), wzh_ref[1], wzl_ref[1])
    fine = []
    for h in range(2):
        total = zf[288 * h : 288 * h + 48]
        for i in range(1, 6):
            total = total + rolled(zf[48 * (6 * h + i) : 48 * (6 * h + i) + 48], 20 * i)
        fine.append(total + bf_ref[:, 128 * h : 128 * h + 128])
    coarse = rolled(zc[0:24], 80)
    for p in range(1, 6):
        coarse = coarse + rolled(zc[24 * p : 24 * p + 24], 80 + 8 * p)

    j = lane % 4
    extra = None
    for h in range(2):
        s = jnp.where(j < 2, zr_ref[h], zo_ref[h])
        d = jnp.where(j < 2, zr_ref[2 + h], zo_ref[2 + h])
        slope = jnp.where(j >= 2, rolled(s, 2), 0.0) - jnp.where(j < 2, rolled(s, 126), 0.0)
        slope = slope + 8.0 * (
            jnp.where(j == 1, rolled(s, 127), 0.0) - jnp.where(j == 2, rolled(s, 1), 0.0)
        )
        part = mm3(along_y(slope * d), mh_ref[h], ml_ref[h])
        extra = part if extra is None else extra + part

    zero8 = jnp.zeros((8, 128), f32)
    zero32 = jnp.zeros((32, 128), f32)
    low = fine[0] + jnp.concatenate([zero32, extra[0:16, 0:128]], 0)
    high = fine[1] + jnp.concatenate([zero32, extra[0:16, 128:256]], 0)
    spread = jnp.concatenate(
        [coarse[0:8], zero8, coarse[8:16], zero8, coarse[16:24] + extra[16:24, 256:384], zero8], 0
    )
    fine_ref[:, 0:128] = low
    fine_ref[:, 128:256] = high
    lane = lanes((48, 128))
    chunk = jnp.where(lane < 40, low, jnp.where(lane < 80, rolled(high, 88), spread))
    for i in range(n):
        chunk_ref[i] = chunk


def project(n, w, f, xr, yr, zr, zo, bent):
    constants = tables()
    return pl.pallas_call(
        project_kernel,
        in_specs=whole(13) + [pl.BlockSpec(memory_space=pltpu.SMEM)],
        out_specs=whole(2),
        out_shape=[
            jax.ShapeDtypeStruct((n, 48, 128), f32),
            jax.ShapeDtypeStruct((48, 256), f32),
        ],
        scratch_shapes=[
            VMEM((68, 80, 128), f32),
            VMEM((64, 48, 128), f32),
            VMEM((64, 24, 128), f32),
            VMEM((12, 48, 128), f32),
            VMEM((6, 24, 128), f32),
        ],
        name="project",
    )(w, f, xr, yr, zr, zo, bent, *(jnp.asarray(c) for c in constants))


def sides(ref, axis):
    n = ref.shape[0]
    i = lax.axis_index(axis)
    return ref[jnp.maximum(i - 1, 0)], i > 0, ref[jnp.minimum(i + 1, n - 1)], i < n - 1


def x_kernel(ny, got_ref, fine_ref, chunk_ref, own_ref, pack_ref):
    n = got_ref.shape[0]
    lane = lanes((24, 128))
    coarse = jnp.zeros((24, 128), f32)
    for j in range(n):
        part = jnp.concatenate([got_ref[j, 16 * a : 16 * a + 8, :] for a in range(3)], 0)
        first, last = max(0, 16 * j - 16), min(16 * n, 16 * j + 32)
        coarse = coarse + jnp.where((lane >= first) & (lane < last), rolled(part, 16 * j - 96), 0.0)
    low, has_low, high, has_high = sides(got_ref, "gx")
    lane = lanes((48, 128))
    middle = (lane >= 40) & (lane < 80)
    own_ref[:, 0:128] = fine_ref[:, 0:128] + jnp.where(middle & has_low, low, 0.0)
    own_ref[:, 128:256] = fine_ref[:, 128:256] + jnp.where(middle & has_high, rolled(high, 40), 0.0)
    pack_ref[0:24, :] = coarse
    for h in range(2):
        for a in range(3):
            at = 24 + 12 * h + 4 * a
            cols = slice(128 * h, 128 * h + 128)
            pack_ref[at : at + 2, :] = own_ref[16 * a : 16 * a + 2, cols]
            pack_ref[at + 2 : at + 4, :] = own_ref[16 * a + 10 : 16 * a + 12, cols]
    for i in range(ny):
        chunk_ref[i] = pack_ref[...]


def x_stage(ny, got, fine):
    return pl.pallas_call(
        functools.partial(x_kernel, ny),
        in_specs=whole(2),
        out_specs=whole(2),
        out_shape=[
            jax.ShapeDtypeStruct((ny, 48, 128), f32),
            jax.ShapeDtypeStruct((48, 256), f32),
        ],
        scratch_shapes=[VMEM((48, 128), f32)],
        name="xstage",
    )(got, fine)


def lane_of(p):
    return 128 * (p // 6), 20 * (p % 6)


def y_kernel(nz, got_ref, fine_ref, chunk_ref, own_ref, sum_ref):
    n = got_ref.shape[0]
    sum_ref[...] = jnp.zeros_like(sum_ref)
    for j in range(n):
        for a in range(3):
            at = 24 * a + 2 * j
            sum_ref[at : at + 6, :] += got_ref[j, 8 * a : 8 * a + 6, :]
    low, has_low, high, has_high = sides(got_ref, "gy")
    own_ref[...] = fine_ref[...]
    for h in range(2):
        cols = slice(128 * h, 128 * h + 128)
        for a in range(3):
            at = 24 + 12 * h + 4 * a
            own_ref[16 * a + 2 : 16 * a + 4, cols] += jnp.where(has_low, low[at + 2 : at + 4], 0.0)
            own_ref[16 * a + 8 : 16 * a + 10, cols] += jnp.where(has_high, high[at : at + 2], 0.0)
    lane = lanes((8, 128))
    border = jnp.zeros((8, 128), f32)
    for a in range(3):
        for p in range(8):
            tile, base = lane_of(p + 2)
            v = own_ref[16 * a + 2 : 16 * a + 10, tile : tile + 128]
            at = 32 * a + 4 * p
            border = jnp.where((lane >= at) & (lane < at + 2), rolled(v, at - base), border)
            border = jnp.where((lane >= at + 2) & (lane < at + 4), rolled(v, at - base - 16), border)
    for i in range(nz):
        for a in range(3):
            chunk_ref[i, 16 * a : 16 * a + 16, :] = sum_ref[24 * a + 2 : 24 * a + 18, :]
        chunk_ref[i, 48:56, :] = border


def y_stage(nz, got, fine):
    return pl.pallas_call(
        functools.partial(y_kernel, nz),
        in_specs=whole(2),
        out_specs=whole(2),
        out_shape=[
            jax.ShapeDtypeStruct((nz, 56, 128), f32),
            jax.ShapeDtypeStruct((48, 256), f32),
        ],
        scratch_shapes=[VMEM((72, 128), f32)],
        name="ystage",
    )(got, fine)


def z_kernel(nx, ny, got_ref, fine_ref, bk_ref, out_fine_ref, out_coarse_ref):
    n = got_ref.shape[0]
    low, has_low, high, has_high = sides(got_ref, "gz")
    low = jnp.where(has_low, low[48:56], 0.0)
    high = jnp.where(has_high, high[48:56], 0.0)
    lane = lanes((8, 128))
    for a in range(3):
        for p in range(8):
            tile, base = lane_of(p + 2)
            v = fine_ref[16 * a + 2 : 16 * a + 10, tile : tile + 128]
            at = 32 * a + 4 * p
            v = v + jnp.where((lane >= base + 2) & (lane < base + 4), rolled(low, base - at), 0.0)
            v = v + jnp.where((lane >= base + 16) & (lane < base + 18), rolled(high, base + 16 - at), 0.0)
            out_fine_ref[a, p] = rolled(v, -(base + 2))[:, 0:16]

    lane = lanes((48, 128))
    k = lane % 8
    parts = [got_ref[m, 0:48, :] for m in range(n)]
    sums = []
    for m in range(n):
        total = parts[m]
        if m > 0:
            total = total + jnp.where(k < 4, rolled(parts[m - 1], -4), 0.0)
        if m < n - 1:
            total = total + jnp.where(k >= 4, rolled(parts[m + 1], 4), 0.0)
        sums.append(jnp.where((k >= 2) & (k < 6), total, 0.0))
    tiles = [rolled(sums[2 * m], -2) + rolled(sums[2 * m + 1], 2) for m in range(n // 2)]
    for p in range(2 * nx):
        total = None
        for m in range(n // 2):
            moved = rolled(tiles[m], 8 * m - 8 * p)
            total = moved if total is None else jnp.where(lane >= 8 * m, moved, total)
        for a in range(3):
            out_coarse_ref[a, p] = total[16 * a : 16 * a + 2 * ny, 0 : 4 * n] + bk_ref[a, p]


def z_stage(nx, ny, got, fine, bent):
    return pl.pallas_call(
        functools.partial(z_kernel, nx, ny),
        in_specs=whole(3),
        out_specs=whole(2),
        out_shape=[
            jax.ShapeDtypeStruct((3, 8, 8, 16), f32),
            jax.ShapeDtypeStruct(bent.shape, f32),
        ],
        name="zstage",
    )(got, fine, bent)


def shifted_up(values, axis):
    return lax.ppermute(values, axis, [(i, i + 1) for i in range(lax.axis_size(axis) - 1)])


def exchanged(chunks, axis):
    return lax.all_to_all(chunks, axis, split_axis=0, concat_axis=0, tiled=True)


def per_device(warped_image, fixed_image, fine_control, coarse_control):
    sizes = tuple(lax.axis_size(n) for n in ("gx", "gy", "gz"))
    xf, yf, zf = faces(warped_image, fixed_image)
    zr = shifted_up(zf, "gz")
    yr = shifted_up(yf, "gy")
    xr = shifted_up(xf, "gx")
    bent_fine, bent_coarse = bend(sizes, fine_control, coarse_control)
    chunk, fine = project(sizes[0], warped_image, fixed_image, xr, yr, zr, zf, bent_fine)
    chunk, fine = x_stage(sizes[1], exchanged(chunk, "gx"), fine)
    chunk, fine = y_stage(sizes[2], exchanged(chunk, "gy"), fine)
    return tuple(z_stage(sizes[0], sizes[1], exchanged(chunk, "gz"), fine, bent_coarse))


def solution(mesh):
    in_specs = (P("gx", "gy", "gz"), P("gx", "gy", "gz"), P(None, "gx", "gy", "gz"), P())
    out_specs = (P(None, "gx", "gy", "gz"), P())
    return jax.shard_map(
        per_device, mesh=mesh, in_specs=in_specs, out_specs=out_specs, check_vma=False
    )
```

```python
import functools

import jax
import jax.numpy as jnp
import numpy as np
from jax import lax
from jax.experimental import pallas as pl
from jax.experimental.pallas import tpu as pltpu
from jax.sharding import PartitionSpec as P

SPF = 8
SPC = 32
BEND = 0.01
f32 = jnp.float32
bf16 = jnp.bfloat16
VMEM = pltpu.VMEM


def spline(t):
    t = np.abs(t)
    inner = 2.0 / 3.0 - t * t + 0.5 * t**3
    outer = (2.0 - t) ** 3 / 6.0
    return np.where(t < 1.0, inner, np.where(t < 2.0, outer, 0.0))


def weights(voxels, points, spacing):
    centre = (np.arange(points) - 2) * spacing + spacing / 2
    return spline((np.asarray(voxels)[:, None] + 0.5 - centre[None, :]) / spacing)


def halves(matrix):
    matrix = np.asarray(matrix, np.float32)
    high = matrix.astype(bf16)
    return high, (matrix - high.astype(np.float32)).astype(bf16)


def split(values):
    high = values.astype(bf16)
    return high, (values - high.astype(f32)).astype(bf16)


def mm(a, b):
    return jnp.dot(a, b, preferred_element_type=f32)


def mm3(values, high, low):
    a, b = split(values)
    return mm(a, high) + mm(b, high) + mm(a, low)


def lanes(shape):
    return lax.broadcasted_iota(jnp.int32, shape, len(shape) - 1)


def rows_of(shape):
    return lax.broadcasted_iota(jnp.int32, shape, len(shape) - 2)


def rolled(values, shift):
    shift %= values.shape[-1]
    return values if shift == 0 else pltpu.roll(values, shift, values.ndim - 1)


def within(mib):
    return pltpu.CompilerParams(vmem_limit_bytes=mib * 2**20)


def whole(n):
    return [pl.BlockSpec(memory_space=VMEM)] * n


STEP = 16
PARTS = 64 // STEP


def faces_kernel(w_hbm, f_hbm, xf_ref, xo_ref, yf_ref, yo_ref, zf_ref, s_ref, d_ref, w_ref, f_ref, sem):
    def copies(g):
        part = pl.ds(g * STEP, STEP)
        return [
            pltpu.make_async_copy(hbm.at[part], ref.at[part], sem.at[i, g])
            for i, (hbm, ref) in enumerate(((w_hbm, w_ref), (f_hbm, f_ref)))
        ]

    for g in range(PARTS):
        for copy in copies(g):
            copy.start()
    lane = lanes((64, 128))
    s_ref[:, 0:8, :] = jnp.zeros((68, 8, 128), f32)
    s_ref[:, 72:80, :] = jnp.zeros((68, 8, 128), f32)
    for x in (0, 1, 66, 67):
        s_ref[x, 8:72, :] = jnp.zeros((64, 128), f32)

    def part(g, carry):
        for copy in copies(g):
            copy.wait()
        packed_s = jnp.zeros((64, 128), f32)
        packed_d = jnp.zeros((64, 128), f32)
        for i in range(STEP):
            x = g * STEP + i
            w = w_ref[x]
            f = f_ref[x]
            s = w + f
            d = w - f
            s_ref[x + 2, 8:72, :] = s
            d_ref[x] = d
            row = pl.ds(x, 1)
            for j in range(2):
                yf_ref[j, row, :] = s[62 + j : 63 + j]
                yf_ref[2 + j, row, :] = d[62 + j : 63 + j]
                yo_ref[j, row, :] = s[j : j + 1]
                yo_ref[2 + j, row, :] = d[j : j + 1]
            here = (lane >= 4 * i) & (lane < 4 * i + 4)
            packed_s = jnp.where(here, rolled(s, 4 * i + 2), packed_s)
            packed_d = jnp.where(here, rolled(d, 4 * i + 2), packed_d)
        half = g // 2

        @pl.when(g % 2 == 0)
        def _():
            zf_ref[half] = packed_s
            zf_ref[2 + half] = packed_d

        @pl.when(g % 2 == 1)
        def _():
            zf_ref[half] = jnp.where(lane < 64, zf_ref[half], rolled(packed_s, 64))
            zf_ref[2 + half] = jnp.where(lane < 64, zf_ref[2 + half], rolled(packed_d, 64))

        return carry

    lax.fori_loop(0, PARTS, part, 0)
    for j in range(2):
        xf_ref[j] = s_ref[64 + j, 8:72, :]
        xf_ref[2 + j] = d_ref[62 + j]
        xo_ref[j] = s_ref[2 + j, 8:72, :]
        xo_ref[2 + j] = d_ref[j]


def faces(w, f):
    shapes = [(4, 64, 128)] * 5 + [(68, 80, 128), (64, 64, 128)]
    return pl.pallas_call(
        faces_kernel,
        in_specs=[pl.BlockSpec(memory_space=pltpu.HBM)] * 2,
        out_specs=whole(7),
        out_shape=[jax.ShapeDtypeStruct(s, f32) for s in shapes],
        scratch_shapes=[
            VMEM((64, 64, 128), f32),
            VMEM((64, 64, 128), f32),
            pltpu.SemaphoreType.DMA((2, PARTS)),
        ],
        compiler_params=within(16),
        name="faces",
    )(*(pltpu.with_memory_space_constraint(v, pltpu.HBM) for v in (w, f)))


def bend_kernel(sizes, c_ref, k_ref, bf_ref, bk_ref, u_ref, a_ref, b_ref):
    nx, ny, nz = sizes
    ix, iy, iz = (lax.axis_index(n) for n in ("gx", "gy", "gz"))
    u_ref[...] = jnp.zeros_like(u_ref)
    for a in range(3):
        for p in range(8):
            at = 20 * (p + 2) + 2
            u_ref[a * 16 + 2 : a * 16 + 10, at : at + 16] = c_ref[a, p]
    lane = lanes((48, 256))
    row = rows_of((48, 256)) % 16
    gp = lane // 20 - 2 + 8 * ix
    gr = lane % 20 - 2 + 16 * iz
    gq = row - 2 + 8 * iy
    inside = (gp >= 0) & (gp < 8 * nx) & (gq >= 0) & (gq < 8 * ny) & (gr >= 0) & (gr < 16 * nz)

    def around(u):
        total = pltpu.roll(u, 1, 0) + pltpu.roll(u, 47, 0)
        for shift in (1, 255, 20, 236):
            total = total + pltpu.roll(u, shift, 1)
        return total - 6.0 * u

    u = around(u_ref[...])
    u = around(jnp.where(inside, u, 0.0)) * BEND
    keep = lanes((48, 128)) < 120
    bf_ref[:, 0:128] = jnp.where(keep, u[:, 0:128], 0.0)
    bf_ref[:, 128:256] = jnp.where(keep, pltpu.roll(u, 136, 1)[:, 0:128], 0.0)

    kx, ky, kz = 2 * nx, 2 * ny, 4 * nz
    a_ref[...] = jnp.zeros_like(a_ref)
    b_ref[...] = jnp.zeros_like(b_ref)
    for a in range(3):
        for p in range(kx):
            a_ref[a, p + 1, 8 : 8 + ky, 0:kz] = k_ref[a, p]
    grid = lanes((ky, 128)) < kz

    def star(ref, a, p):
        mid = ref[a, p + 1, 8 : 8 + ky, :]
        total = ref[a, p, 8 : 8 + ky, :] + ref[a, p + 2, 8 : 8 + ky, :]
        total = total + ref[a, p + 1, 7 : 7 + ky, :] + ref[a, p + 1, 9 : 9 + ky, :]
        total = total + rolled(mid, 1) + rolled(mid, 127)
        return total - 6.0 * mid

    for a in range(3):
        for p in range(kx):
            b_ref[a, p + 1, 8 : 8 + ky, :] = jnp.where(grid, star(a_ref, a, p), 0.0)
    for a in range(3):
        for p in range(kx):
            bk_ref[a, p] = (star(b_ref, a, p) * BEND)[:, 0:kz]


def bend(sizes, control, coarse):
    nx, ny, nz = sizes
    grid = (3, 2 * nx + 2, 2 * ny + 16, 128)
    return pl.pallas_call(
        functools.partial(bend_kernel, sizes),
        in_specs=whole(2),
        out_specs=whole(2),
        out_shape=[
            jax.ShapeDtypeStruct((48, 256), f32),
            jax.ShapeDtypeStruct(coarse.shape, f32),
        ],
        scratch_shapes=[VMEM((48, 256), f32), VMEM(grid, f32), VMEM(grid, f32)],
        cost_estimate=pl.CostEstimate(flops=4000000, bytes_accessed=1000000, transcendentals=0),
        compiler_params=within(8),
        name="bend",
    )(control, coarse)


@functools.cache
def tables():
    own = np.arange(64)
    cross = np.arange(-2, 2)
    wy = np.zeros((24, 64))
    wy[0:12] = weights(own, 12, SPF).T
    wy[16:22] = weights(own, 6, SPC).T
    high, low = halves(wy)
    left = np.concatenate(
        [np.concatenate([high, high], 1), np.concatenate([low, np.zeros_like(low)], 1)], 0
    )
    wc = np.zeros((8, 8, 128), np.float32)
    for j in range(4):
        wc[j, :, :] = weights(cross, 12, SPF)[j, 0:8, None]
        wc[4 + j, 0:6, :] = weights(cross, 6, SPC)[j, :, None]
    fine_scale = SPF**-1.5 / 24.0
    coarse_scale = SPC**-1.5 / 24.0
    wz = np.zeros((2, 128, 128))
    wz[0, :, 0:20] = weights(np.arange(128), 20, SPF) * fine_scale
    wz[1, :, 0:8] = weights(np.arange(128), 8, SPC) * coarse_scale
    wz_high, wz_low = halves(wz)
    m = np.zeros((2, 128, 384))
    fx, cx = weights(own, 12, SPF), weights(own, 6, SPC)
    fz = weights(cross, 20, SPF) * fine_scale
    cz = weights(cross, 8, SPC) * coarse_scale
    for x in range(64):
        for j in range(4):
            line = m[x // 32, 4 * (x % 32) + j]
            for p in range(12):
                at = 128 * (p // 6) + 20 * (p % 6)
                line[at : at + 20] = fx[x, p] * fz[j]
            for p in range(6):
                at = 256 + 80 + 8 * p
                line[at : at + 8] = cx[x, p] * cz[j]
    m_high, m_low = halves(m)
    coarse_x = weights(own, 6, SPC).astype(np.float32).reshape(-1)
    return left, wc, wz_high, wz_low, m_high, m_low, coarse_x


def along(left, force):
    high, low = split(force)
    both = mm(left, jnp.concatenate([high, low], 0))
    return both[0:24] + both[24:48]


def interior_kernel(s_ref, d_ref, left_ref, cx_ref, af_ref, ac_ref, tf_ref, tc_ref):
    fx = weights(np.arange(8), 5, SPF)
    left = left_ref[...]
    lane = lanes((64, 128))

    def layer(x, carry):
        s = s_ref[x + 2, 8:72, :]
        d = d_ref[x]
        below, above = s_ref[x + 1, 8:72, :], s_ref[x + 3, 8:72, :]
        f0 = (s_ref[x, 8:72, :] - s_ref[x + 4, 8:72, :]) + 8.0 * (above - below)
        f1 = (s_ref[x + 2, 6:70, :] - s_ref[x + 2, 10:74, :]) + 8.0 * (
            s_ref[x + 2, 9:73, :] - s_ref[x + 2, 7:71, :]
        )
        f2 = jnp.where(lane >= 2, rolled(s, 2), 0.0) - jnp.where(lane < 126, rolled(s, 126), 0.0)
        f2 = f2 + 8.0 * (
            jnp.where(lane < 127, rolled(s, 127), 0.0) - jnp.where(lane >= 1, rolled(s, 1), 0.0)
        )
        t = along(left, jnp.concatenate([f0 * d, f1 * d, f2 * d], 1))
        for a in range(3):
            cols = slice(128 * a, 128 * a + 128)
            tf_ref[x, 16 * a : 16 * a + 16, :] = t[0:16, cols]
            tc_ref[x, 8 * a : 8 * a + 8, :] = t[16:24, cols]
        return carry

    lax.fori_loop(0, 64, layer, 0, unroll=8)

    af_ref[...] = jnp.zeros_like(af_ref)
    ac_ref[...] = jnp.zeros_like(ac_ref)

    def block(b, carry):
        for k in range(5):
            total = None
            for r in range(8):
                weight = float(fx[r, k])
                if weight == 0.0:
                    continue
                term = weight * tf_ref[8 * b + r]
                total = term if total is None else total + term
            af_ref[b + k] += total
        for k in range(6):
            total = None
            for r in range(8):
                term = cx_ref[(8 * b + r) * 6 + k] * tc_ref[8 * b + r]
                total = term if total is None else total + term
            ac_ref[k] += total
        return carry

    lax.fori_loop(0, 8, block, 0)


def interior(s, d):
    left, *_, coarse_x = tables()
    return pl.pallas_call(
        interior_kernel,
        in_specs=whole(3) + [pl.BlockSpec(memory_space=pltpu.SMEM)],
        out_specs=whole(2),
        out_shape=[
            jax.ShapeDtypeStruct((12, 48, 128), f32),
            jax.ShapeDtypeStruct((6, 24, 128), f32),
        ],
        scratch_shapes=[VMEM((64, 48, 128), f32), VMEM((64, 24, 128), f32)],
        cost_estimate=pl.CostEstimate(flops=40000000, bytes_accessed=4000000, transcendentals=0),
        compiler_params=within(16),
        name="interior",
    )(s, d, jnp.asarray(left), jnp.asarray(coarse_x))


def crossing(first, second):
    sm2, sm1, dm2, dm1 = (first[i] for i in range(4))
    s0, s1, d0, d1 = (second[i] for i in range(4))
    return [-s0 * dm2, (8.0 * s0 - s1) * dm1, (sm2 - 8.0 * sm1) * d0, sm1 * d1]


def finish_kernel(
    af_ref, ac_ref, xr_ref, xo_ref, yr_ref, yo_ref, zr_ref, zo_ref, bf_ref, left_ref, wc_ref, wzh_ref, wzl_ref, mh_ref, ml_ref,
    chunk_ref, fine_ref, sf_ref, sc_ref,
):
    n = chunk_ref.shape[0]
    edge_f = weights(np.arange(-2, 2), 4, SPF)
    edge_c = weights(np.arange(-2, 2), 4, SPC)
    left = left_ref[...]
    lane = lanes((64, 128))

    edge = along(left, jnp.concatenate(crossing(xr_ref, xo_ref), 1))
    sf_ref[...] = af_ref[...]
    sc_ref[...] = ac_ref[...]
    for k in range(4):
        for j in range(4):
            cols = slice(128 * j, 128 * j + 128)
            fine = float(edge_f[j, k]) * edge[0:16, cols]
            coarse = float(edge_c[j, k]) * edge[16:24, cols]
            total_f = fine if j == 0 else total_f + fine
            total_c = coarse if j == 0 else total_c + coarse
        sf_ref[k, 0:16, :] += total_f
        sc_ref[k, 0:8, :] += total_c

    edge = along(left, jnp.concatenate(crossing(yr_ref, yo_ref), 1))
    for p in range(12):
        total = sf_ref[p, 16:24, :]
        for j in range(4):
            total = total + wc_ref[j] * edge[p : p + 1, 128 * j : 128 * j + 128]
        sf_ref[p, 16:24, :] = total
    for p in range(6):
        total = sc_ref[p, 8:16, :]
        for j in range(4):
            total = total + wc_ref[4 + j] * edge[16 + p : 17 + p, 128 * j : 128 * j + 128]
        sc_ref[p, 8:16, :] = total

    zf = mm3(sf_ref[...].reshape(576, 128), wzh_ref[0], wzl_ref[0])
    zc = mm3(sc_ref[...].reshape(144, 128), wzh_ref[1], wzl_ref[1])
    fine = []
    for h in range(2):
        total = zf[288 * h : 288 * h + 48]
        for i in range(1, 6):
            total = total + rolled(zf[48 * (6 * h + i) : 48 * (6 * h + i) + 48], 20 * i)
        fine.append(total + bf_ref[:, 128 * h : 128 * h + 128])
    coarse = rolled(zc[0:24], 80)
    for p in range(1, 6):
        coarse = coarse + rolled(zc[24 * p : 24 * p + 24], 80 + 8 * p)

    j = lane % 4
    extra = None
    for h in range(2):
        s = jnp.where(j < 2, zr_ref[h], zo_ref[h])
        d = jnp.where(j < 2, zr_ref[2 + h], zo_ref[2 + h])
        slope = jnp.where(j >= 2, rolled(s, 2), 0.0) - jnp.where(j < 2, rolled(s, 126), 0.0)
        slope = slope + 8.0 * (
            jnp.where(j == 1, rolled(s, 127), 0.0) - jnp.where(j == 2, rolled(s, 1), 0.0)
        )
        part = mm3(along(left, slope * d), mh_ref[h], ml_ref[h])
        extra = part if extra is None else extra + part

    zero8 = jnp.zeros((8, 128), f32)
    zero32 = jnp.zeros((32, 128), f32)
    low = fine[0] + jnp.concatenate([zero32, extra[0:16, 0:128]], 0)
    high = fine[1] + jnp.concatenate([zero32, extra[0:16, 128:256]], 0)
    spread = jnp.concatenate(
        [coarse[0:8], zero8, coarse[8:16], zero8, coarse[16:24] + extra[16:24, 256:384], zero8], 0
    )
    fine_ref[:, 0:128] = low
    fine_ref[:, 128:256] = high
    lane = lanes((48, 128))
    chunk = jnp.where(lane < 40, low, jnp.where(lane < 80, rolled(high, 88), spread))
    for i in range(n):
        chunk_ref[i] = chunk


def finish(n, *values):
    constants = tables()[:-1]
    return pl.pallas_call(
        finish_kernel,
        in_specs=whole(15),
        out_specs=whole(2),
        out_shape=[
            jax.ShapeDtypeStruct((n, 48, 128), f32),
            jax.ShapeDtypeStruct((48, 256), f32),
        ],
        scratch_shapes=[VMEM((12, 48, 128), f32), VMEM((6, 24, 128), f32)],
        compiler_params=within(12),
        name="finish",
    )(*values, *(jnp.asarray(c) for c in constants))


def sides(ref, axis):
    n = ref.shape[0]
    i = lax.axis_index(axis)
    return ref[jnp.maximum(i - 1, 0)], i > 0, ref[jnp.minimum(i + 1, n - 1)], i < n - 1


def x_kernel(ny, got_ref, fine_ref, chunk_ref, own_ref, pack_ref):
    n = got_ref.shape[0]
    lane = lanes((24, 128))
    coarse = jnp.zeros((24, 128), f32)
    for j in range(n):
        part = jnp.concatenate([got_ref[j, 16 * a : 16 * a + 8, :] for a in range(3)], 0)
        first, last = max(0, 16 * j - 16), min(16 * n, 16 * j + 32)
        coarse = coarse + jnp.where((lane >= first) & (lane < last), rolled(part, 16 * j - 96), 0.0)
    low, has_low, high, has_high = sides(got_ref, "gx")
    lane = lanes((48, 128))
    middle = (lane >= 40) & (lane < 80)
    own_ref[:, 0:128] = fine_ref[:, 0:128] + jnp.where(middle & has_low, low, 0.0)
    own_ref[:, 128:256] = fine_ref[:, 128:256] + jnp.where(middle & has_high, rolled(high, 40), 0.0)
    pack_ref[0:24, :] = coarse
    for h in range(2):
        for a in range(3):
            at = 24 + 12 * h + 4 * a
            cols = slice(128 * h, 128 * h + 128)
            pack_ref[at : at + 2, :] = own_ref[16 * a : 16 * a + 2, cols]
            pack_ref[at + 2 : at + 4, :] = own_ref[16 * a + 10 : 16 * a + 12, cols]
    for i in range(ny):
        chunk_ref[i] = pack_ref[...]


def x_stage(ny, got, fine):
    return pl.pallas_call(
        functools.partial(x_kernel, ny),
        in_specs=whole(2),
        out_specs=whole(2),
        out_shape=[
            jax.ShapeDtypeStruct((ny, 48, 128), f32),
            jax.ShapeDtypeStruct((48, 256), f32),
        ],
        scratch_shapes=[VMEM((48, 128), f32)],
        compiler_params=within(4),
        name="xstage",
    )(got, fine)


def lane_of(p):
    return 128 * (p // 6), 20 * (p % 6)


def y_kernel(nz, got_ref, fine_ref, chunk_ref, own_ref, sum_ref):
    n = got_ref.shape[0]
    sum_ref[...] = jnp.zeros_like(sum_ref)
    for j in range(n):
        for a in range(3):
            at = 24 * a + 2 * j
            sum_ref[at : at + 6, :] += got_ref[j, 8 * a : 8 * a + 6, :]
    low, has_low, high, has_high = sides(got_ref, "gy")
    own_ref[...] = fine_ref[...]
    for h in range(2):
        cols = slice(128 * h, 128 * h + 128)
        for a in range(3):
            at = 24 + 12 * h + 4 * a
            own_ref[16 * a + 2 : 16 * a + 4, cols] += jnp.where(has_low, low[at + 2 : at + 4], 0.0)
            own_ref[16 * a + 8 : 16 * a + 10, cols] += jnp.where(has_high, high[at : at + 2], 0.0)
    lane = lanes((8, 128))
    border = jnp.zeros((8, 128), f32)
    for a in range(3):
        for p in range(8):
            tile, base = lane_of(p + 2)
            v = own_ref[16 * a + 2 : 16 * a + 10, tile : tile + 128]
            at = 32 * a + 4 * p
            border = jnp.where((lane >= at) & (lane < at + 2), rolled(v, at - base), border)
            border = jnp.where((lane >= at + 2) & (lane < at + 4), rolled(v, at - base - 16), border)
    for i in range(nz):
        for a in range(3):
            chunk_ref[i, 16 * a : 16 * a + 16, :] = sum_ref[24 * a + 2 : 24 * a + 18, :]
        chunk_ref[i, 48:56, :] = border


def y_stage(nz, got, fine):
    return pl.pallas_call(
        functools.partial(y_kernel, nz),
        in_specs=whole(2),
        out_specs=whole(2),
        out_shape=[
            jax.ShapeDtypeStruct((nz, 56, 128), f32),
            jax.ShapeDtypeStruct((48, 256), f32),
        ],
        scratch_shapes=[VMEM((72, 128), f32)],
        compiler_params=within(4),
        name="ystage",
    )(got, fine)


def z_kernel(nx, ny, got_ref, fine_ref, bk_ref, out_fine_ref, out_coarse_ref):
    n = got_ref.shape[0]
    low, has_low, high, has_high = sides(got_ref, "gz")
    low = jnp.where(has_low, low[48:56], 0.0)
    high = jnp.where(has_high, high[48:56], 0.0)
    lane = lanes((8, 128))
    for a in range(3):
        for p in range(8):
            tile, base = lane_of(p + 2)
            v = fine_ref[16 * a + 2 : 16 * a + 10, tile : tile + 128]
            at = 32 * a + 4 * p
            v = v + jnp.where((lane >= base + 2) & (lane < base + 4), rolled(low, base - at), 0.0)
            v = v + jnp.where((lane >= base + 16) & (lane < base + 18), rolled(high, base + 16 - at), 0.0)
            out_fine_ref[a, p] = rolled(v, -(base + 2))[:, 0:16]

    lane = lanes((48, 128))
    k = lane % 8
    parts = [got_ref[m, 0:48, :] for m in range(n)]
    sums = []
    for m in range(n):
        total = parts[m]
        if m > 0:
            total = total + jnp.where(k < 4, rolled(parts[m - 1], -4), 0.0)
        if m < n - 1:
            total = total + jnp.where(k >= 4, rolled(parts[m + 1], 4), 0.0)
        sums.append(jnp.where((k >= 2) & (k < 6), total, 0.0))
    tiles = [rolled(sums[2 * m], -2) + rolled(sums[2 * m + 1], 2) for m in range(n // 2)]
    for p in range(2 * nx):
        total = None
        for m in range(n // 2):
            moved = rolled(tiles[m], 8 * m - 8 * p)
            total = moved if total is None else jnp.where(lane >= 8 * m, moved, total)
        for a in range(3):
            out_coarse_ref[a, p] = total[16 * a : 16 * a + 2 * ny, 0 : 4 * n] + bk_ref[a, p]


def z_stage(nx, ny, got, fine, bent):
    return pl.pallas_call(
        functools.partial(z_kernel, nx, ny),
        in_specs=whole(3),
        out_specs=whole(2),
        out_shape=[
            jax.ShapeDtypeStruct((3, 8, 8, 16), f32),
            jax.ShapeDtypeStruct(bent.shape, f32),
        ],
        compiler_params=within(6),
        name="zstage",
    )(got, fine, bent)


def shifted_up(values, axis):
    return lax.ppermute(values, axis, [(i, i + 1) for i in range(lax.axis_size(axis) - 1)])


def exchanged(chunks, axis):
    return lax.all_to_all(chunks, axis, split_axis=0, concat_axis=0, tiled=True)


def per_device(warped_image, fixed_image, fine_control, coarse_control):
    sizes = tuple(lax.axis_size(n) for n in ("gx", "gy", "gz"))
    xf, xo, yf, yo, zf, s, d = faces(warped_image, fixed_image)
    zr = shifted_up(zf, "gz")
    yr = shifted_up(yf, "gy")
    xr = shifted_up(xf, "gx")
    bent_fine, bent_coarse = bend(sizes, fine_control, coarse_control)
    fine, coarse = interior(s, d)
    chunk, fine = finish(sizes[0], fine, coarse, xr, xo, yr, yo, zr, zf, bent_fine)
    chunk, fine = x_stage(sizes[1], exchanged(chunk, "gx"), fine)
    chunk, fine = y_stage(sizes[2], exchanged(chunk, "gy"), fine)
    return tuple(z_stage(sizes[0], sizes[1], exchanged(chunk, "gz"), fine, bent_coarse))


def solution(mesh):
    in_specs = (P("gx", "gy", "gz"), P("gx", "gy", "gz"), P(None, "gx", "gy", "gz"), P())
    out_specs = (P(None, "gx", "gy", "gz"), P())
    return jax.shard_map(
        per_device, mesh=mesh, in_specs=in_specs, out_specs=out_specs, check_vma=False
    )
```

```python
import functools

import jax
import jax.numpy as jnp
import numpy as np
from jax import lax
from jax.experimental import pallas as pl
from jax.experimental.pallas import tpu as pltpu
from jax.sharding import PartitionSpec as P

SPF = 8
SPC = 32
BEND = 0.01
f32 = jnp.float32
bf16 = jnp.bfloat16
VMEM = pltpu.VMEM


def spline(t):
    t = np.abs(t)
    inner = 2.0 / 3.0 - t * t + 0.5 * t**3
    outer = (2.0 - t) ** 3 / 6.0
    return np.where(t < 1.0, inner, np.where(t < 2.0, outer, 0.0))


def weights(voxels, points, spacing):
    centre = (np.arange(points) - 2) * spacing + spacing / 2
    return spline((np.asarray(voxels)[:, None] + 0.5 - centre[None, :]) / spacing)


def halves(matrix):
    matrix = np.asarray(matrix, np.float32)
    high = matrix.astype(bf16)
    return high, (matrix - high.astype(np.float32)).astype(bf16)


def split(values):
    high = values.astype(bf16)
    return high, (values - high.astype(f32)).astype(bf16)


def mm(a, b):
    return jnp.dot(a, b, preferred_element_type=f32)


def mm3(values, high, low):
    a, b = split(values)
    return mm(a, high) + mm(b, high) + mm(a, low)


def lanes(shape):
    return lax.broadcasted_iota(jnp.int32, shape, len(shape) - 1)


def rows_of(shape):
    return lax.broadcasted_iota(jnp.int32, shape, len(shape) - 2)


def rolled(values, shift):
    shift %= values.shape[-1]
    return values if shift == 0 else pltpu.roll(values, shift, values.ndim - 1)


def within(mib):
    return pltpu.CompilerParams(vmem_limit_bytes=mib * 2**20)


def whole(n):
    return [pl.BlockSpec(memory_space=VMEM)] * n


STEP = 8
PARTS = 64 // STEP


def faces_kernel(w_hbm, f_hbm, xf_ref, xo_ref, yf_ref, yo_ref, zf_ref, s_ref, t_ref, d_ref, w_ref, f_ref, sem):
    def copies(g):
        part = pl.ds(g * STEP, STEP)
        return [
            pltpu.make_async_copy(hbm.at[part], ref.at[part], sem.at[i, g])
            for i, (hbm, ref) in enumerate(((w_hbm, w_ref), (f_hbm, f_ref)))
        ]

    for g in range(PARTS):
        for copy in copies(g):
            copy.start()
    lane = lanes((64, 128))
    for ref in (s_ref, t_ref):
        ref[:, 0:8, :] = jnp.zeros((68, 8, 128), f32)
        ref[:, 72:80, :] = jnp.zeros((68, 8, 128), f32)
        for x in (0, 1, 66, 67):
            ref[x, 8:72, :] = jnp.zeros((64, 128), f32)

    def part(g, carry):
        for copy in copies(g):
            copy.wait()
        packed_s = jnp.zeros((64, 128), f32)
        packed_d = jnp.zeros((64, 128), f32)
        for i in range(STEP):
            x = g * STEP + i
            w = w_ref[x]
            f = f_ref[x]
            s = w + f
            d = w - f
            s_ref[x + 2, 8:72, :] = s
            t_ref[x + 2, 8:72, :] = 8.0 * s
            d_ref[x] = d
            row = pl.ds(x, 1)
            for j in range(2):
                yf_ref[j, row, :] = s[62 + j : 63 + j]
                yf_ref[2 + j, row, :] = d[62 + j : 63 + j]
                yo_ref[j, row, :] = s[j : j + 1]
                yo_ref[2 + j, row, :] = d[j : j + 1]
            here = (lane >= 4 * i) & (lane < 4 * i + 4)
            packed_s = jnp.where(here, rolled(s, 4 * i + 2), packed_s)
            packed_d = jnp.where(here, rolled(d, 4 * i + 2), packed_d)
        half, quarter = g // 4, g % 4
        here = lane // 32 == quarter
        for i, packed in ((half, packed_s), (2 + half, packed_d)):
            zf_ref[i] = jnp.where(here, pltpu.roll(packed, 32 * quarter, 1), zf_ref[i])
        return carry

    lax.fori_loop(0, PARTS, part, 0)
    for j in range(2):
        xf_ref[j] = s_ref[64 + j, 8:72, :]
        xf_ref[2 + j] = d_ref[62 + j]
        xo_ref[j] = s_ref[2 + j, 8:72, :]
        xo_ref[2 + j] = d_ref[j]


def faces(w, f):
    shapes = [(4, 64, 128)] * 5 + [(68, 80, 128)] * 2 + [(64, 64, 128)]
    return pl.pallas_call(
        faces_kernel,
        in_specs=[pl.BlockSpec(memory_space=pltpu.HBM)] * 2,
        out_specs=whole(8),
        out_shape=[jax.ShapeDtypeStruct(s, f32) for s in shapes],
        scratch_shapes=[
            VMEM((64, 64, 128), f32),
            VMEM((64, 64, 128), f32),
            pltpu.SemaphoreType.DMA((2, PARTS)),
        ],
        compiler_params=within(16),
        name="faces",
    )(*(pltpu.with_memory_space_constraint(v, pltpu.HBM) for v in (w, f)))


def bend_kernel(sizes, c_ref, k_ref, bf_ref, bk_ref, u_ref, k2_ref):
    nx, ny, nz = sizes
    ix, iy, iz = (lax.axis_index(n) for n in ("gx", "gy", "gz"))
    u_ref[...] = jnp.zeros_like(u_ref)
    for a in range(3):
        for p in range(8):
            at = 20 * (p + 2) + 2
            u_ref[a * 16 + 2 : a * 16 + 10, at : at + 16] = c_ref[a, p]
    lane = lanes((48, 256))
    row = rows_of((48, 256)) % 16
    gp = lane // 20 - 2 + 8 * ix
    gr = lane % 20 - 2 + 16 * iz
    gq = row - 2 + 8 * iy
    inside = (gp >= 0) & (gp < 8 * nx) & (gq >= 0) & (gq < 8 * ny) & (gr >= 0) & (gr < 16 * nz)

    def around(u, step):
        total = pltpu.roll(u, 1, 0) + pltpu.roll(u, u.shape[0] - 1, 0)
        for shift in (1, -1, step, -step):
            total = total + rolled(u, shift)
        return total - 6.0 * u

    u = around(u_ref[...], 20)
    u = around(jnp.where(inside, u, 0.0), 20) * BEND
    keep = lanes((48, 128)) < 120
    bf_ref[:, 0:128] = jnp.where(keep, u[:, 0:128], 0.0)
    bf_ref[:, 128:256] = jnp.where(keep, pltpu.roll(u, 136, 1)[:, 0:128], 0.0)

    kx, ky, kz = 2 * nx, 2 * ny, 4 * nz
    k2_ref[...] = jnp.zeros_like(k2_ref)
    parts = []
    for a in range(3):
        total = None
        for p in range(6):
            i = 6 * a + p
            k2_ref[i, 0:ky, 0:kz] = k_ref[a, jnp.clip(2 * ix - 2 + p, 0, kx - 1)]
            tile = pltpu.roll(k2_ref[i], (18 - 2 * iy) % 16, 0)[0:8]
            tile = pltpu.roll(tile, (130 - 4 * iz + 8 * p) % 128, 1)
            total = tile if p == 0 else jnp.where(lanes((8, 128)) // 8 == p, tile, total)
        parts.append(total)
    lane = lanes((24, 128))
    row = rows_of((24, 128)) % 8
    gp, gq, gr = 2 * ix - 2 + lane // 8, 2 * iy - 2 + row, 4 * iz - 2 + lane % 8
    inside = (gp >= 0) & (gp < kx) & (gq >= 0) & (gq < ky) & (gr >= 0) & (gr < kz) & (lane < 48)
    u = jnp.where(inside, jnp.concatenate(parts, 0), 0.0)
    u = around(jnp.where(inside, around(u, 8), 0.0), 8) * BEND
    own = (lane // 16 == 1) & (row // 2 == 1) & ((lane % 8 + 2) // 4 == 1)
    bk_ref[...] = rolled(jnp.where(own, u, 0.0), 80)


def bend(sizes, control, coarse):
    return pl.pallas_call(
        functools.partial(bend_kernel, sizes),
        in_specs=whole(2),
        out_specs=whole(2),
        out_shape=[
            jax.ShapeDtypeStruct((48, 256), f32),
            jax.ShapeDtypeStruct((24, 128), f32),
        ],
        scratch_shapes=[VMEM((48, 256), f32), VMEM((18, 16, 128), f32)],
        cost_estimate=pl.CostEstimate(flops=4000000, bytes_accessed=1000000, transcendentals=0),
        compiler_params=within(8),
        name="bend",
    )(control, coarse)


@functools.cache
def tables():
    own = np.arange(64)
    cross = np.arange(-2, 2)
    wy = np.zeros((24, 64))
    wy[0:12] = weights(own, 12, SPF).T
    wy[16:22] = weights(own, 6, SPC).T
    high, low = halves(wy)
    left = np.concatenate(
        [np.concatenate([high, high], 1), np.concatenate([low, np.zeros_like(low)], 1)], 0
    )
    wc = np.zeros((8, 8, 128), np.float32)
    for j in range(4):
        wc[j, :, :] = weights(cross, 12, SPF)[j, 0:8, None]
        wc[4 + j, 0:6, :] = weights(cross, 6, SPC)[j, :, None]
    fine_scale = SPF**-1.5 / 24.0
    coarse_scale = SPC**-1.5 / 24.0
    wz = np.zeros((2, 128, 128))
    wz[0, :, 0:20] = weights(np.arange(128), 20, SPF) * fine_scale
    wz[1, :, 0:8] = weights(np.arange(128), 8, SPC) * coarse_scale
    wz_high, wz_low = halves(wz)
    m = np.zeros((4, 128, 384))
    fx, cx = weights(own, 12, SPF), weights(own, 6, SPC)
    fz = weights(cross, 20, SPF) * fine_scale
    cz = weights(cross, 8, SPC) * coarse_scale
    fz = np.concatenate([fz, weights(np.arange(126, 128), 20, SPF) * fine_scale])
    cz = np.concatenate([cz, weights(np.arange(126, 128), 8, SPC) * coarse_scale])
    for x in range(64):
        for j in range(6):
            line = m[x // 32 + 2 * (j // 4), 4 * (x % 32) + j % 4]
            for p in range(12):
                at = 128 * (p // 6) + 20 * (p % 6)
                line[at : at + 20] = fx[x, p] * fz[j]
            for p in range(6):
                at = 256 + 80 + 8 * p
                line[at : at + 8] = cx[x, p] * cz[j]
    m_high, m_low = halves(m)
    return left, wc, wz_high, wz_low, m_high, m_low


def along(left, force):
    high, low = split(force)
    both = mm(left, jnp.concatenate([high, low], 0))
    return both[0:24] + both[24:48]


def interior_kernel(s_ref, t_ref, d_ref, left_ref, af_ref, ac_ref, tf_ref, tc_ref):
    fx = weights(np.arange(8), 5, SPF)
    cx = weights(np.arange(64), 6, SPC)
    left = left_ref[...]

    def force(x):
        d = d_ref[x]
        f0 = (s_ref[x, 8:72, :] - s_ref[x + 4, 8:72, :]) + (t_ref[x + 3, 8:72, :] - t_ref[x + 1, 8:72, :])
        s, t = s_ref.at[x + 2], t_ref.at[x + 2]
        f1 = (s[6:70, :] - s[10:74, :]) + (t[9:73, :] - t[7:71, :])
        s, t = s[8:72, :], t[8:72, :]
        f2 = (rolled(s, 2) - rolled(s, 126)) + (rolled(t, 127) - rolled(t, 1))
        return [f0 * d, f1 * d, f2 * d]

    def layers(b):
        for i in range(0, 8, 2):
            section = along(left, jnp.concatenate(force(8 * b + i) + force(8 * b + i + 1), 1))
            for k in range(6):
                at, a = 8 * b + i + k // 3, k % 3
                cols = slice(128 * k, 128 * k + 128)
                tf_ref[at, 16 * a : 16 * a + 16, :] = section[0:16, cols]
                tc_ref[at, 8 * a : 8 * a + 8, :] = section[16:24, cols]

    def block(b):
        for k in range(5):
            total = af_ref[b + k]
            for r in range(8):
                weight = float(fx[r, k])
                if weight != 0.0:
                    total = total + weight * tf_ref[8 * b + r]
            af_ref[b + k] = total
        for k in range((b + 2) // 4, (b + 2) // 4 + 4):
            total = ac_ref[k]
            for r in range(8):
                total = total + float(cx[8 * b + r, k]) * tc_ref[8 * b + r]
            ac_ref[k] = total

    af_ref[...] = jnp.zeros_like(af_ref)
    ac_ref[...] = jnp.zeros_like(ac_ref)
    for b in range(8):
        layers(b)
        if b > 0:
            block(b - 1)
    block(7)


def interior(s, s8, d):
    left = tables()[0]
    return pl.pallas_call(
        interior_kernel,
        in_specs=whole(4),
        out_specs=whole(2),
        out_shape=[
            jax.ShapeDtypeStruct((12, 48, 128), f32),
            jax.ShapeDtypeStruct((6, 24, 128), f32),
        ],
        scratch_shapes=[VMEM((64, 48, 128), f32), VMEM((64, 24, 128), f32)],
        cost_estimate=pl.CostEstimate(flops=40000000, bytes_accessed=4000000, transcendentals=0),
        compiler_params=within(16),
        name="interior",
    )(s, s8, d, jnp.asarray(left))


def crossing(first, second):
    sm2, sm1, dm2, dm1 = (first[i] for i in range(4))
    s0, s1, d0, d1 = (second[i] for i in range(4))
    return [-s0 * dm2, (8.0 * s0 - s1) * dm1, (sm2 - 8.0 * sm1) * d0, sm1 * d1]


def finish_kernel(
    af_ref, ac_ref, xr_ref, xo_ref, yr_ref, yo_ref, zr_ref, zo_ref, bf_ref, bk_ref, left_ref, wc_ref, wzh_ref, wzl_ref, mh_ref, ml_ref,
    chunk_ref, fine_ref, sf_ref, sc_ref,
):
    n = chunk_ref.shape[0]
    edge_f = weights(np.arange(-2, 2), 4, SPF)
    edge_c = weights(np.arange(-2, 2), 4, SPC)
    left = left_ref[...]
    lane = lanes((64, 128))

    edge = along(left, jnp.concatenate(crossing(xr_ref, xo_ref), 1))
    sf_ref[...] = af_ref[...]
    sc_ref[...] = ac_ref[...]
    for k in range(4):
        for j in range(4):
            cols = slice(128 * j, 128 * j + 128)
            fine = float(edge_f[j, k]) * edge[0:16, cols]
            coarse = float(edge_c[j, k]) * edge[16:24, cols]
            total_f = fine if j == 0 else total_f + fine
            total_c = coarse if j == 0 else total_c + coarse
        sf_ref[k, 0:16, :] += total_f
        sc_ref[k, 0:8, :] += total_c

    edge = along(left, jnp.concatenate(crossing(yr_ref, yo_ref), 1))
    for p in range(12):
        total = sf_ref[p, 16:24, :]
        for j in range(4):
            total = total + wc_ref[j] * edge[p : p + 1, 128 * j : 128 * j + 128]
        sf_ref[p, 16:24, :] = total
    for p in range(6):
        total = sc_ref[p, 8:16, :]
        for j in range(4):
            total = total + wc_ref[4 + j] * edge[16 + p : 17 + p, 128 * j : 128 * j + 128]
        sc_ref[p, 8:16, :] = total

    zf = mm3(sf_ref[...].reshape(576, 128), wzh_ref[0], wzl_ref[0])
    zc = mm3(sc_ref[...].reshape(144, 128), wzh_ref[1], wzl_ref[1])
    fine = []
    for h in range(2):
        total = zf[288 * h : 288 * h + 48]
        for i in range(1, 6):
            total = total + rolled(zf[48 * (6 * h + i) : 48 * (6 * h + i) + 48], 20 * i)
        fine.append(total + bf_ref[:, 128 * h : 128 * h + 128])
    coarse = bk_ref[...] + rolled(zc[0:24], 80)
    for p in range(1, 6):
        coarse = coarse + rolled(zc[24 * p : 24 * p + 24], 80 + 8 * p)

    j = lane % 4
    extra = None
    for h in range(2):
        s = jnp.where(j < 2, zr_ref[h] - zo_ref[h], zo_ref[h])
        d = jnp.where(j < 2, zr_ref[2 + h], zo_ref[2 + h])
        slope = jnp.where(j >= 2, rolled(s, 2), 0.0) - jnp.where(j < 2, rolled(s, 126), 0.0)
        slope = slope + 8.0 * (
            jnp.where(j == 1, rolled(s, 127), 0.0) - jnp.where(j == 2, rolled(s, 1), 0.0)
        )
        wrapped = jnp.where(j < 2, -slope * zo_ref[2 + h], 0.0)
        part = along(left, jnp.concatenate([slope * d, wrapped], 1))
        part = mm3(part[:, 0:128], mh_ref[h], ml_ref[h]) + mm3(part[:, 128:256], mh_ref[2 + h], ml_ref[2 + h])
        extra = part if extra is None else extra + part

    zero8 = jnp.zeros((8, 128), f32)
    zero32 = jnp.zeros((32, 128), f32)
    low = fine[0] + jnp.concatenate([zero32, extra[0:16, 0:128]], 0)
    high = fine[1] + jnp.concatenate([zero32, extra[0:16, 128:256]], 0)
    spread = jnp.concatenate(
        [coarse[0:8], zero8, coarse[8:16], zero8, coarse[16:24] + extra[16:24, 256:384], zero8], 0
    )
    fine_ref[:, 0:128] = low
    fine_ref[:, 128:256] = high
    lane = lanes((48, 128))
    chunk = jnp.where(lane < 40, low, jnp.where(lane < 80, rolled(high, 88), spread))
    for i in range(n):
        chunk_ref[i] = chunk


def finish(n, *values):
    constants = tables()
    return pl.pallas_call(
        finish_kernel,
        in_specs=whole(16),
        out_specs=whole(2),
        out_shape=[
            jax.ShapeDtypeStruct((n, 48, 128), f32),
            jax.ShapeDtypeStruct((48, 256), f32),
        ],
        scratch_shapes=[VMEM((12, 48, 128), f32), VMEM((6, 24, 128), f32)],
        compiler_params=within(12),
        name="finish",
    )(*values, *(jnp.asarray(c) for c in constants))


def sides(ref, axis):
    n = ref.shape[0]
    i = lax.axis_index(axis)
    return ref[jnp.maximum(i - 1, 0)], i > 0, ref[jnp.minimum(i + 1, n - 1)], i < n - 1


def x_kernel(ny, got_ref, fine_ref, chunk_ref, own_ref, pack_ref):
    n = got_ref.shape[0]
    lane = lanes((24, 128))
    coarse = jnp.zeros((24, 128), f32)
    for j in range(n):
        part = jnp.concatenate([got_ref[j, 16 * a : 16 * a + 8, :] for a in range(3)], 0)
        first, last = max(0, 16 * j - 16), min(16 * n, 16 * j + 32)
        coarse = coarse + jnp.where((lane >= first) & (lane < last), rolled(part, 16 * j - 96), 0.0)
    low, has_low, high, has_high = sides(got_ref, "gx")
    lane = lanes((48, 128))
    middle = (lane >= 40) & (lane < 80)
    own_ref[:, 0:128] = fine_ref[:, 0:128] + jnp.where(middle & has_low, low, 0.0)
    own_ref[:, 128:256] = fine_ref[:, 128:256] + jnp.where(middle & has_high, rolled(high, 40), 0.0)
    pack_ref[0:24, :] = coarse
    for h in range(2):
        for a in range(3):
            at = 24 + 12 * h + 4 * a
            cols = slice(128 * h, 128 * h + 128)
            pack_ref[at : at + 2, :] = own_ref[16 * a : 16 * a + 2, cols]
            pack_ref[at + 2 : at + 4, :] = own_ref[16 * a + 10 : 16 * a + 12, cols]
    for i in range(ny):
        chunk_ref[i] = pack_ref[...]


def x_stage(ny, got, fine):
    return pl.pallas_call(
        functools.partial(x_kernel, ny),
        in_specs=whole(2),
        out_specs=whole(2),
        out_shape=[
            jax.ShapeDtypeStruct((ny, 48, 128), f32),
            jax.ShapeDtypeStruct((48, 256), f32),
        ],
        scratch_shapes=[VMEM((48, 128), f32)],
        compiler_params=within(4),
        name="xstage",
    )(got, fine)


def lane_of(p):
    return 128 * (p // 6), 20 * (p % 6)


def y_kernel(nz, got_ref, fine_ref, chunk_ref, own_ref, sum_ref):
    n = got_ref.shape[0]
    sum_ref[...] = jnp.zeros_like(sum_ref)
    for j in range(n):
        for a in range(3):
            at = 24 * a + 2 * j
            sum_ref[at : at + 6, :] += got_ref[j, 8 * a : 8 * a + 6, :]
    low, has_low, high, has_high = sides(got_ref, "gy")
    own_ref[...] = fine_ref[...]
    for h in range(2):
        cols = slice(128 * h, 128 * h + 128)
        for a in range(3):
            at = 24 + 12 * h + 4 * a
            own_ref[16 * a + 2 : 16 * a + 4, cols] += jnp.where(has_low, low[at + 2 : at + 4], 0.0)
            own_ref[16 * a + 8 : 16 * a + 10, cols] += jnp.where(has_high, high[at : at + 2], 0.0)
    lane = lanes((8, 128))
    border = jnp.zeros((8, 128), f32)
    for a in range(3):
        for p in range(8):
            tile, base = lane_of(p + 2)
            v = own_ref[16 * a + 2 : 16 * a + 10, tile : tile + 128]
            at = 32 * a + 4 * p
            border = jnp.where((lane >= at) & (lane < at + 2), rolled(v, at - base), border)
            border = jnp.where((lane >= at + 2) & (lane < at + 4), rolled(v, at - base - 16), border)
    for i in range(nz):
        for a in range(3):
            chunk_ref[i, 16 * a : 16 * a + 16, :] = sum_ref[24 * a + 2 : 24 * a + 18, :]
        chunk_ref[i, 48:56, :] = border


def y_stage(nz, got, fine):
    return pl.pallas_call(
        functools.partial(y_kernel, nz),
        in_specs=whole(2),
        out_specs=whole(2),
        out_shape=[
            jax.ShapeDtypeStruct((nz, 56, 128), f32),
            jax.ShapeDtypeStruct((48, 256), f32),
        ],
        scratch_shapes=[VMEM((72, 128), f32)],
        compiler_params=within(4),
        name="ystage",
    )(got, fine)


def z_kernel(nx, ny, got_ref, fine_ref, out_fine_ref, out_coarse_ref):
    n = got_ref.shape[0]
    low, has_low, high, has_high = sides(got_ref, "gz")
    low = jnp.where(has_low, low[48:56], 0.0)
    high = jnp.where(has_high, high[48:56], 0.0)
    lane = lanes((8, 128))
    for a in range(3):
        for p in range(8):
            tile, base = lane_of(p + 2)
            v = fine_ref[16 * a + 2 : 16 * a + 10, tile : tile + 128]
            at = 32 * a + 4 * p
            v = v + jnp.where((lane >= base + 2) & (lane < base + 4), rolled(low, base - at), 0.0)
            v = v + jnp.where((lane >= base + 16) & (lane < base + 18), rolled(high, base + 16 - at), 0.0)
            out_fine_ref[a, p] = rolled(v, -(base + 2))[:, 0:16]

    lane = lanes((48, 128))
    k = lane % 8
    parts = [got_ref[m, 0:48, :] for m in range(n)]
    tiles = []
    for m in range(0, n, 2):
        total = jnp.where(k < 6, rolled(parts[m], -2), 0.0) + jnp.where(k >= 2, rolled(parts[m + 1], 2), 0.0)
        if m > 0:
            total = total + jnp.where(k < 2, rolled(parts[m - 1], -6), 0.0)
        if m + 2 < n:
            total = total + jnp.where(k >= 6, rolled(parts[m + 2], 6), 0.0)
        tiles.append(total)
    per = len(tiles)
    slot = lane // 8 % per
    for h in range(per):
        total = rolled(tiles[0], -8 * h)
        for m in range(1, per):
            total = jnp.where(slot == m, rolled(tiles[m], 8 * (m - h)), total)
        for g in range(2 * nx // per):
            points = rolled(total, -8 * per * g)
            for a in range(3):
                out_coarse_ref[a, per * g + h] = points[16 * a : 16 * a + 2 * ny, 0 : 4 * n]


def z_stage(sizes, got, fine):
    nx, ny, nz = sizes
    return pl.pallas_call(
        functools.partial(z_kernel, nx, ny),
        in_specs=whole(2),
        out_specs=whole(2),
        out_shape=[
            jax.ShapeDtypeStruct((3, 8, 8, 16), f32),
            jax.ShapeDtypeStruct((3, 2 * nx, 2 * ny, 4 * nz), f32),
        ],
        compiler_params=within(6),
        name="zstage",
    )(got, fine)


def shifted_up(values, axis):
    return lax.ppermute(values, axis, [(i, i + 1) for i in range(lax.axis_size(axis) - 1)])


def exchanged(chunks, axis):
    return lax.all_to_all(chunks, axis, split_axis=0, concat_axis=0, tiled=True)


def per_device(warped_image, fixed_image, fine_control, coarse_control):
    sizes = tuple(lax.axis_size(n) for n in ("gx", "gy", "gz"))
    xf, xo, yf, yo, zf, s, s8, d = faces(warped_image, fixed_image)
    zr = shifted_up(zf, "gz")
    yr = shifted_up(yf, "gy")
    xr = shifted_up(xf, "gx")
    bent_fine, bent_coarse = bend(sizes, fine_control, coarse_control)
    fine, coarse = interior(s, s8, d)
    chunk, fine = finish(sizes[0], fine, coarse, xr, xo, yr, yo, zr, zf, bent_fine, bent_coarse)
    chunk, fine = x_stage(sizes[1], exchanged(chunk, "gx"), fine)
    chunk, fine = y_stage(sizes[2], exchanged(chunk, "gy"), fine)
    return tuple(z_stage(sizes, exchanged(chunk, "gz"), fine))


def solution(mesh):
    in_specs = (P("gx", "gy", "gz"), P("gx", "gy", "gz"), P(None, "gx", "gy", "gz"), P())
    out_specs = (P(None, "gx", "gy", "gz"), P())
    return jax.shard_map(
        per_device, mesh=mesh, in_specs=in_specs, out_specs=out_specs, check_vma=False
    )
```

```python
import functools

import jax
import jax.numpy as jnp
import numpy as np
from jax import lax
from jax.experimental import pallas as pl
from jax.experimental.pallas import tpu as pltpu
from jax.sharding import PartitionSpec as P

SPF = 8
SPC = 32
BEND = 0.01
f32 = jnp.float32
bf16 = jnp.bfloat16
VMEM = pltpu.VMEM


def spline(t):
    t = np.abs(t)
    inner = 2.0 / 3.0 - t * t + 0.5 * t**3
    outer = (2.0 - t) ** 3 / 6.0
    return np.where(t < 1.0, inner, np.where(t < 2.0, outer, 0.0))


def weights(voxels, points, spacing):
    centre = (np.arange(points) - 2) * spacing + spacing / 2
    return spline((np.asarray(voxels)[:, None] + 0.5 - centre[None, :]) / spacing)


def halves(matrix):
    matrix = np.asarray(matrix, np.float32)
    high = matrix.astype(bf16)
    return high, (matrix - high.astype(np.float32)).astype(bf16)


def split(values):
    high = values.astype(bf16)
    return high, (values - high.astype(f32)).astype(bf16)


def mm(a, b):
    return jnp.dot(a, b, preferred_element_type=f32)


def mm3(values, high, low):
    a, b = split(values)
    return mm(a, high) + mm(b, high) + mm(a, low)


def lanes(shape):
    return lax.broadcasted_iota(jnp.int32, shape, len(shape) - 1)


def rows_of(shape):
    return lax.broadcasted_iota(jnp.int32, shape, len(shape) - 2)


def rolled(values, shift):
    shift %= values.shape[-1]
    return values if shift == 0 else pltpu.roll(values, shift, values.ndim - 1)


def within(mib):
    return pltpu.CompilerParams(vmem_limit_bytes=mib * 2**20)


def whole(n):
    return [pl.BlockSpec(memory_space=VMEM)] * n


STEP = 16
PARTS = 64 // STEP


def faces_kernel(w_hbm, f_hbm, xf_ref, xo_ref, yf_ref, yo_ref, zf_ref, zo_ref, s_ref, t_ref, d_ref, w_ref, f_ref, sem):
    def copies(g):
        part = pl.ds(g * STEP, STEP)
        return [
            pltpu.make_async_copy(hbm.at[part], ref.at[part], sem.at[i, g])
            for i, (hbm, ref) in enumerate(((w_hbm, w_ref), (f_hbm, f_ref)))
        ]

    for g in range(PARTS):
        for copy in copies(g):
            copy.start()
    lane = lanes((64, 128))
    for ref in (s_ref, t_ref):
        ref[:, 0:8, :] = jnp.zeros((68, 8, 128), f32)
        ref[:, 72:80, :] = jnp.zeros((68, 8, 128), f32)
        for x in (0, 1, 66, 67):
            ref[x, 8:72, :] = jnp.zeros((64, 128), f32)

    def part(g):
        for copy in copies(g):
            copy.wait()
        packed_s = jnp.zeros((64, 128), f32)
        packed_d = jnp.zeros((64, 128), f32)
        for i in range(STEP):
            x = g * STEP + i
            w = w_ref[x]
            f = f_ref[x]
            s = w + f
            d = w - f
            s_ref[x + 2, 8:72, :] = s
            t_ref[x + 2, 8:72, :] = 8.0 * s
            d_ref[x] = d
            row = pl.ds(x, 1)
            for j in range(2):
                yf_ref[j, row, :] = s[62 + j : 63 + j]
                yf_ref[2 + j, row, :] = d[62 + j : 63 + j]
                yo_ref[j, row, :] = s[j : j + 1]
                yo_ref[2 + j, row, :] = d[j : j + 1]
            here = (lane >= 4 * i) & (lane < 4 * i + 4)
            packed_s = jnp.where(here, rolled(s, 4 * i + 2), packed_s)
            packed_d = jnp.where(here, rolled(d, 4 * i + 2), packed_d)
        for ref, packed in ((zo_ref, packed_s), (zo_ref.at[2:4], packed_d)):
            half = g // 2
            ref[half] = packed if g % 2 == 0 else jnp.where(lane < 64, ref[half], rolled(packed, 64))

    for g in range(PARTS):
        part(g)
    for j in range(2):
        xf_ref[j] = s_ref[64 + j, 8:72, :]
        xf_ref[2 + j] = d_ref[62 + j]
        xo_ref[j] = s_ref[2 + j, 8:72, :]
        xo_ref[2 + j] = d_ref[j]
        zf_ref[j] = jnp.where(lane % 4 < 2, zo_ref[2 * j], rolled(zo_ref[2 * j + 1], 2))


def faces(w, f):
    shapes = [(4, 64, 128)] * 4 + [(2, 64, 128), (4, 64, 128)] + [(68, 80, 128)] * 2 + [(64, 64, 128)]
    return pl.pallas_call(
        faces_kernel,
        in_specs=[pl.BlockSpec(memory_space=pltpu.HBM)] * 2,
        out_specs=whole(9),
        out_shape=[jax.ShapeDtypeStruct(s, f32) for s in shapes],
        scratch_shapes=[
            VMEM((64, 64, 128), f32),
            VMEM((64, 64, 128), f32),
            pltpu.SemaphoreType.DMA((2, PARTS)),
        ],
        compiler_params=within(16),
        name="faces",
    )(*(pltpu.with_memory_space_constraint(v, pltpu.HBM) for v in (w, f)))


def bend_kernel(sizes, c_ref, k_ref, bf_ref, bk_ref, u_ref, k2_ref):
    nx, ny, nz = sizes
    ix, iy, iz = (lax.axis_index(n) for n in ("gx", "gy", "gz"))
    u_ref[...] = jnp.zeros_like(u_ref)
    for a in range(3):
        for p in range(8):
            at = 20 * (p + 2) + 2
            u_ref[a * 16 + 2 : a * 16 + 10, at : at + 16] = c_ref[a, p]
    lane = lanes((48, 256))
    row = rows_of((48, 256)) % 16
    gp = lane // 20 - 2 + 8 * ix
    gr = lane % 20 - 2 + 16 * iz
    gq = row - 2 + 8 * iy
    inside = (gp >= 0) & (gp < 8 * nx) & (gq >= 0) & (gq < 8 * ny) & (gr >= 0) & (gr < 16 * nz)

    def around(u, step):
        total = pltpu.roll(u, 1, 0) + pltpu.roll(u, u.shape[0] - 1, 0)
        for shift in (1, -1, step, -step):
            total = total + rolled(u, shift)
        return total - 6.0 * u

    u = around(u_ref[...], 20)
    u = around(jnp.where(inside, u, 0.0), 20) * BEND
    keep = lanes((48, 128)) < 120
    bf_ref[:, 0:128] = jnp.where(keep, u[:, 0:128], 0.0)
    bf_ref[:, 128:256] = jnp.where(keep, pltpu.roll(u, 136, 1)[:, 0:128], 0.0)

    kx, ky, kz = 2 * nx, 2 * ny, 4 * nz
    k2_ref[...] = jnp.zeros_like(k2_ref)
    parts = []
    for a in range(3):
        total = None
        for p in range(6):
            i = 6 * a + p
            k2_ref[i, 0:ky, 0:kz] = k_ref[a, jnp.clip(2 * ix - 2 + p, 0, kx - 1)]
            tile = pltpu.roll(k2_ref[i], (18 - 2 * iy) % 16, 0)[0:8]
            tile = pltpu.roll(tile, (130 - 4 * iz + 8 * p) % 128, 1)
            total = tile if p == 0 else jnp.where(lanes((8, 128)) // 8 == p, tile, total)
        parts.append(total)
    lane = lanes((24, 128))
    row = rows_of((24, 128)) % 8
    gp, gq, gr = 2 * ix - 2 + lane // 8, 2 * iy - 2 + row, 4 * iz - 2 + lane % 8
    inside = (gp >= 0) & (gp < kx) & (gq >= 0) & (gq < ky) & (gr >= 0) & (gr < kz) & (lane < 48)
    u = jnp.where(inside, jnp.concatenate(parts, 0), 0.0)
    u = around(jnp.where(inside, around(u, 8), 0.0), 8) * BEND
    own = (lane // 16 == 1) & (row // 2 == 1) & ((lane % 8 + 2) // 4 == 1)
    bk_ref[...] = rolled(jnp.where(own, u, 0.0), 80)


def bend(sizes, control, coarse):
    return pl.pallas_call(
        functools.partial(bend_kernel, sizes),
        in_specs=whole(2),
        out_specs=whole(2),
        out_shape=[
            jax.ShapeDtypeStruct((48, 256), f32),
            jax.ShapeDtypeStruct((24, 128), f32),
        ],
        scratch_shapes=[VMEM((48, 256), f32), VMEM((18, 16, 128), f32)],
        cost_estimate=pl.CostEstimate(flops=4000000, bytes_accessed=1000000, transcendentals=0),
        compiler_params=within(8),
        name="bend",
    )(control, coarse)


@functools.cache
def tables():
    own = np.arange(64)
    cross = np.arange(-2, 2)
    wy = np.zeros((24, 64))
    wy[0:12] = weights(own, 12, SPF).T
    wy[16:22] = weights(own, 6, SPC).T
    high, low = halves(wy)
    left = np.concatenate(
        [np.concatenate([high, high], 1), np.concatenate([low, np.zeros_like(low)], 1)], 0
    )
    wc = np.zeros((8, 8, 128), np.float32)
    for j in range(4):
        wc[j, :, :] = weights(cross, 12, SPF)[j, 0:8, None]
        wc[4 + j, 0:6, :] = weights(cross, 6, SPC)[j, :, None]
    fine_scale = SPF**-1.5 / 24.0
    coarse_scale = SPC**-1.5 / 24.0
    wz = np.zeros((2, 128, 128))
    wz[0, :, 0:20] = weights(np.arange(128), 20, SPF) * fine_scale
    wz[1, :, 0:8] = weights(np.arange(128), 8, SPC) * coarse_scale
    wz_high, wz_low = halves(wz)
    m = np.zeros((4, 128, 384))
    fx, cx = weights(own, 12, SPF), weights(own, 6, SPC)
    fz = weights(cross, 20, SPF) * fine_scale
    cz = weights(cross, 8, SPC) * coarse_scale
    fz = np.concatenate([fz, weights(np.arange(126, 128), 20, SPF) * fine_scale])
    cz = np.concatenate([cz, weights(np.arange(126, 128), 8, SPC) * coarse_scale])
    for x in range(64):
        for j in range(6):
            line = m[x // 32 + 2 * (j // 4), 4 * (x % 32) + j % 4]
            for p in range(12):
                at = 128 * (p // 6) + 20 * (p % 6)
                line[at : at + 20] = fx[x, p] * fz[j]
            for p in range(6):
                at = 256 + 80 + 8 * p
                line[at : at + 8] = cx[x, p] * cz[j]
    m_high, m_low = halves(m)
    return left, wc, wz_high, wz_low, m_high, m_low


def along(left, force):
    high, low = split(force)
    both = mm(left, jnp.concatenate([high, low], 0))
    return both[0:24] + both[24:48]


def interior_kernel(s_ref, t_ref, d_ref, left_ref, af_ref, ac_ref, tf_ref, tc_ref):
    fx = weights(np.arange(8), 5, SPF)
    cx = weights(np.arange(64), 6, SPC)
    left = left_ref[...]

    def force(x):
        d = d_ref[x]
        f0 = (s_ref[x, 8:72, :] - s_ref[x + 4, 8:72, :]) + (t_ref[x + 3, 8:72, :] - t_ref[x + 1, 8:72, :])
        s, t = s_ref.at[x + 2], t_ref.at[x + 2]
        f1 = (s[6:70, :] - s[10:74, :]) + (t[9:73, :] - t[7:71, :])
        s, t = s[8:72, :], t[8:72, :]
        f2 = (rolled(s, 2) - rolled(s, 126)) + (rolled(t, 127) - rolled(t, 1))
        return [f0 * d, f1 * d, f2 * d]

    def layers(b):
        for i in range(0, 8, 2):
            section = along(left, jnp.concatenate(force(8 * b + i) + force(8 * b + i + 1), 1))
            for k in range(6):
                at, a = 8 * b + i + k // 3, k % 3
                cols = slice(128 * k, 128 * k + 128)
                tf_ref[at, 16 * a : 16 * a + 16, :] = section[0:16, cols]
                tc_ref[at, 8 * a : 8 * a + 8, :] = section[16:24, cols]

    def block(b):
        for k in range(5):
            total = af_ref[b + k]
            for r in range(8):
                weight = float(fx[r, k])
                if weight != 0.0:
                    total = total + weight * tf_ref[8 * b + r]
            af_ref[b + k] = total
        for k in range((b + 2) // 4, (b + 2) // 4 + 4):
            total = ac_ref[k]
            for r in range(8):
                total = total + float(cx[8 * b + r, k]) * tc_ref[8 * b + r]
            ac_ref[k] = total

    af_ref[...] = jnp.zeros_like(af_ref)
    ac_ref[...] = jnp.zeros_like(ac_ref)
    for b in range(8):
        layers(b)
        if b > 0:
            block(b - 1)
    block(7)


def interior(s, s8, d):
    left = tables()[0]
    return pl.pallas_call(
        interior_kernel,
        in_specs=whole(4),
        out_specs=whole(2),
        out_shape=[
            jax.ShapeDtypeStruct((12, 48, 128), f32),
            jax.ShapeDtypeStruct((6, 24, 128), f32),
        ],
        scratch_shapes=[VMEM((64, 48, 128), f32), VMEM((64, 24, 128), f32)],
        cost_estimate=pl.CostEstimate(flops=40000000, bytes_accessed=4000000, transcendentals=0),
        compiler_params=within(16),
        name="interior",
    )(s, s8, d, jnp.asarray(left))


def crossing(first, second):
    sm2, sm1, dm2, dm1 = (first[i] for i in range(4))
    s0, s1, d0, d1 = (second[i] for i in range(4))
    return [-s0 * dm2, (8.0 * s0 - s1) * dm1, (sm2 - 8.0 * sm1) * d0, sm1 * d1]


def finish_kernel(
    af_ref, ac_ref, xr_ref, xo_ref, yr_ref, yo_ref, zr_ref, zo_ref, bf_ref, bk_ref, left_ref, wc_ref, wzh_ref, wzl_ref, mh_ref, ml_ref,
    chunk_ref, fine_ref, sf_ref, sc_ref,
):
    n = chunk_ref.shape[0]
    edge_f = weights(np.arange(-2, 2), 4, SPF)
    edge_c = weights(np.arange(-2, 2), 4, SPC)
    left = left_ref[...]
    lane = lanes((64, 128))

    edge = along(left, jnp.concatenate(crossing(xr_ref, xo_ref), 1))
    sf_ref[...] = af_ref[...]
    sc_ref[...] = ac_ref[...]
    for k in range(4):
        for j in range(4):
            cols = slice(128 * j, 128 * j + 128)
            fine = float(edge_f[j, k]) * edge[0:16, cols]
            coarse = float(edge_c[j, k]) * edge[16:24, cols]
            total_f = fine if j == 0 else total_f + fine
            total_c = coarse if j == 0 else total_c + coarse
        sf_ref[k, 0:16, :] += total_f
        sc_ref[k, 0:8, :] += total_c

    edge = along(left, jnp.concatenate(crossing(yr_ref, yo_ref), 1))
    for p in range(12):
        total = sf_ref[p, 16:24, :]
        for j in range(4):
            total = total + wc_ref[j] * edge[p : p + 1, 128 * j : 128 * j + 128]
        sf_ref[p, 16:24, :] = total
    for p in range(6):
        total = sc_ref[p, 8:16, :]
        for j in range(4):
            total = total + wc_ref[4 + j] * edge[16 + p : 17 + p, 128 * j : 128 * j + 128]
        sc_ref[p, 8:16, :] = total

    zf = mm3(sf_ref[...].reshape(576, 128), wzh_ref[0], wzl_ref[0])
    zc = mm3(sc_ref[...].reshape(144, 128), wzh_ref[1], wzl_ref[1])
    fine = []
    for h in range(2):
        total = zf[288 * h : 288 * h + 48]
        for i in range(1, 6):
            total = total + rolled(zf[48 * (6 * h + i) : 48 * (6 * h + i) + 48], 20 * i)
        fine.append(total + bf_ref[:, 128 * h : 128 * h + 128])
    coarse = bk_ref[...] + rolled(zc[0:24], 80)
    for p in range(1, 6):
        coarse = coarse + rolled(zc[24 * p : 24 * p + 24], 80 + 8 * p)

    j = lane % 4
    extra = None
    for h in range(2):
        s = jnp.where(j < 2, rolled(zr_ref[0], -2 * h) - zo_ref[h], zo_ref[h])
        d = jnp.where(j < 2, rolled(zr_ref[1], -2 * h), zo_ref[2 + h])
        slope = jnp.where(j >= 2, rolled(s, 2), 0.0) - jnp.where(j < 2, rolled(s, 126), 0.0)
        slope = slope + 8.0 * (
            jnp.where(j == 1, rolled(s, 127), 0.0) - jnp.where(j == 2, rolled(s, 1), 0.0)
        )
        wrapped = jnp.where(j < 2, -slope * zo_ref[2 + h], 0.0)
        part = along(left, jnp.concatenate([slope * d, wrapped], 1))
        part = mm3(part[:, 0:128], mh_ref[h], ml_ref[h]) + mm3(part[:, 128:256], mh_ref[2 + h], ml_ref[2 + h])
        extra = part if extra is None else extra + part

    zero8 = jnp.zeros((8, 128), f32)
    zero32 = jnp.zeros((32, 128), f32)
    low = fine[0] + jnp.concatenate([zero32, extra[0:16, 0:128]], 0)
    high = fine[1] + jnp.concatenate([zero32, extra[0:16, 128:256]], 0)
    spread = jnp.concatenate(
        [coarse[0:8], zero8, coarse[8:16], zero8, coarse[16:24] + extra[16:24, 256:384], zero8], 0
    )
    fine_ref[:, 0:128] = low
    fine_ref[:, 128:256] = high
    lane = lanes((48, 128))
    chunk = jnp.where(lane < 40, low, jnp.where(lane < 80, rolled(high, 88), spread))
    for i in range(n):
        chunk_ref[i] = chunk


def finish(n, *values):
    constants = tables()
    return pl.pallas_call(
        finish_kernel,
        in_specs=whole(16),
        out_specs=whole(2),
        out_shape=[
            jax.ShapeDtypeStruct((n, 48, 128), f32),
            jax.ShapeDtypeStruct((48, 256), f32),
        ],
        scratch_shapes=[VMEM((12, 48, 128), f32), VMEM((6, 24, 128), f32)],
        compiler_params=within(12),
        name="finish",
    )(*values, *(jnp.asarray(c) for c in constants))


def sides(ref, axis):
    n = ref.shape[0]
    i = lax.axis_index(axis)
    return ref[jnp.maximum(i - 1, 0)], i > 0, ref[jnp.minimum(i + 1, n - 1)], i < n - 1


def x_kernel(ny, got_ref, fine_ref, chunk_ref, own_ref, pack_ref):
    n = got_ref.shape[0]
    lane = lanes((24, 128))
    coarse = jnp.zeros((24, 128), f32)
    for j in range(n):
        part = jnp.concatenate([got_ref[j, 16 * a : 16 * a + 8, :] for a in range(3)], 0)
        first, last = max(0, 16 * j - 16), min(16 * n, 16 * j + 32)
        coarse = coarse + jnp.where((lane >= first) & (lane < last), rolled(part, 16 * j - 96), 0.0)
    low, has_low, high, has_high = sides(got_ref, "gx")
    lane = lanes((48, 128))
    middle = (lane >= 40) & (lane < 80)
    own_ref[:, 0:128] = fine_ref[:, 0:128] + jnp.where(middle & has_low, low, 0.0)
    own_ref[:, 128:256] = fine_ref[:, 128:256] + jnp.where(middle & has_high, rolled(high, 40), 0.0)
    pack_ref[0:24, :] = coarse
    for h in range(2):
        for a in range(3):
            at = 24 + 12 * h + 4 * a
            cols = slice(128 * h, 128 * h + 128)
            pack_ref[at : at + 2, :] = own_ref[16 * a : 16 * a + 2, cols]
            pack_ref[at + 2 : at + 4, :] = own_ref[16 * a + 10 : 16 * a + 12, cols]
    for i in range(ny):
        chunk_ref[i] = pack_ref[...]


def x_stage(ny, got, fine):
    return pl.pallas_call(
        functools.partial(x_kernel, ny),
        in_specs=whole(2),
        out_specs=whole(2),
        out_shape=[
            jax.ShapeDtypeStruct((ny, 48, 128), f32),
            jax.ShapeDtypeStruct((48, 256), f32),
        ],
        scratch_shapes=[VMEM((48, 128), f32)],
        compiler_params=within(4),
        name="xstage",
    )(got, fine)


def lane_of(p):
    return 128 * (p // 6), 20 * (p % 6)


def y_kernel(nz, got_ref, fine_ref, chunk_ref, own_ref, sum_ref):
    n = got_ref.shape[0]
    sum_ref[...] = jnp.zeros_like(sum_ref)
    for j in range(n):
        for a in range(3):
            at = 24 * a + 2 * j
            sum_ref[at : at + 6, :] += got_ref[j, 8 * a : 8 * a + 6, :]
    low, has_low, high, has_high = sides(got_ref, "gy")
    own_ref[...] = fine_ref[...]
    for h in range(2):
        cols = slice(128 * h, 128 * h + 128)
        for a in range(3):
            at = 24 + 12 * h + 4 * a
            own_ref[16 * a + 2 : 16 * a + 4, cols] += jnp.where(has_low, low[at + 2 : at + 4], 0.0)
            own_ref[16 * a + 8 : 16 * a + 10, cols] += jnp.where(has_high, high[at : at + 2], 0.0)
    lane = lanes((8, 128))
    border = jnp.zeros((8, 128), f32)
    for a in range(3):
        for p in range(8):
            tile, base = lane_of(p + 2)
            v = own_ref[16 * a + 2 : 16 * a + 10, tile : tile + 128]
            at = 32 * a + 4 * p
            border = jnp.where((lane >= at) & (lane < at + 2), rolled(v, at - base), border)
            border = jnp.where((lane >= at + 2) & (lane < at + 4), rolled(v, at - base - 16), border)
    for i in range(nz):
        for a in range(3):
            chunk_ref[i, 16 * a : 16 * a + 16, :] = sum_ref[24 * a + 2 : 24 * a + 18, :]
        chunk_ref[i, 48:56, :] = border


def y_stage(nz, got, fine):
    return pl.pallas_call(
        functools.partial(y_kernel, nz),
        in_specs=whole(2),
        out_specs=whole(2),
        out_shape=[
            jax.ShapeDtypeStruct((nz, 56, 128), f32),
            jax.ShapeDtypeStruct((48, 256), f32),
        ],
        scratch_shapes=[VMEM((72, 128), f32)],
        compiler_params=within(4),
        name="ystage",
    )(got, fine)


def z_kernel(nx, ny, got_ref, fine_ref, out_fine_ref, out_coarse_ref):
    n = got_ref.shape[0]
    low, has_low, high, has_high = sides(got_ref, "gz")
    low = jnp.where(has_low, low[48:56], 0.0)
    high = jnp.where(has_high, high[48:56], 0.0)
    lane = lanes((8, 128))
    for a in range(3):
        for p in range(8):
            tile, base = lane_of(p + 2)
            v = fine_ref[16 * a + 2 : 16 * a + 10, tile : tile + 128]
            at = 32 * a + 4 * p
            v = v + jnp.where((lane >= base + 2) & (lane < base + 4), rolled(low, base - at), 0.0)
            v = v + jnp.where((lane >= base + 16) & (lane < base + 18), rolled(high, base + 16 - at), 0.0)
            out_fine_ref[a, p] = rolled(v, -(base + 2))[:, 0:16]

    lane = lanes((48, 128))
    k = lane % 8
    parts = [got_ref[m, 0:48, :] for m in range(n)]
    tiles = []
    for m in range(0, n, 2):
        total = jnp.where(k < 6, rolled(parts[m], -2), 0.0) + jnp.where(k >= 2, rolled(parts[m + 1], 2), 0.0)
        if m > 0:
            total = total + jnp.where(k < 2, rolled(parts[m - 1], -6), 0.0)
        if m + 2 < n:
            total = total + jnp.where(k >= 6, rolled(parts[m + 2], 6), 0.0)
        tiles.append(total)
    per = len(tiles)
    slot = lane // 8 % per
    for h in range(per):
        total = rolled(tiles[0], -8 * h)
        for m in range(1, per):
            total = jnp.where(slot == m, rolled(tiles[m], 8 * (m - h)), total)
        for g in range(2 * nx // per):
            points = rolled(total, -8 * per * g)
            for a in range(3):
                out_coarse_ref[a, per * g + h] = points[16 * a : 16 * a + 2 * ny, 0 : 4 * n]


def z_stage(sizes, got, fine):
    nx, ny, nz = sizes
    return pl.pallas_call(
        functools.partial(z_kernel, nx, ny),
        in_specs=whole(2),
        out_specs=whole(2),
        out_shape=[
            jax.ShapeDtypeStruct((3, 8, 8, 16), f32),
            jax.ShapeDtypeStruct((3, 2 * nx, 2 * ny, 4 * nz), f32),
        ],
        compiler_params=within(6),
        name="zstage",
    )(got, fine)


def shifted_up(values, axis):
    return lax.ppermute(values, axis, [(i, i + 1) for i in range(lax.axis_size(axis) - 1)])


def exchanged(chunks, axis):
    return lax.all_to_all(chunks, axis, split_axis=0, concat_axis=0, tiled=True)


def per_device(warped_image, fixed_image, fine_control, coarse_control):
    sizes = tuple(lax.axis_size(n) for n in ("gx", "gy", "gz"))
    xf, xo, yf, yo, zf, zo, s, s8, d = faces(warped_image, fixed_image)
    yr = shifted_up(yf, "gy")
    zr = shifted_up(zf, "gz")
    xr = shifted_up(xf, "gx")
    bent_fine, bent_coarse = bend(sizes, fine_control, coarse_control)
    fine, coarse = interior(s, s8, d)
    chunk, fine = finish(sizes[0], fine, coarse, xr, xo, yr, yo, zr, zo, bent_fine, bent_coarse)
    chunk, fine = x_stage(sizes[1], exchanged(chunk, "gx"), fine)
    chunk, fine = y_stage(sizes[2], exchanged(chunk, "gy"), fine)
    return tuple(z_stage(sizes, exchanged(chunk, "gz"), fine))


def solution(mesh):
    in_specs = (P("gx", "gy", "gz"), P("gx", "gy", "gz"), P(None, "gx", "gy", "gz"), P())
    out_specs = (P(None, "gx", "gy", "gz"), P())
    return jax.shard_map(
        per_device, mesh=mesh, in_specs=in_specs, out_specs=out_specs, check_vma=False
    )
```

```python
import functools

import jax
import jax.numpy as jnp
import numpy as np
from jax import lax
from jax.experimental import pallas as pl
from jax.experimental.pallas import tpu as pltpu
from jax.sharding import PartitionSpec as P

SPF = 8
SPC = 32
BEND = 0.01
f32 = jnp.float32
bf16 = jnp.bfloat16
VMEM = pltpu.VMEM


def spline(t):
    t = np.abs(t)
    inner = 2.0 / 3.0 - t * t + 0.5 * t**3
    outer = (2.0 - t) ** 3 / 6.0
    return np.where(t < 1.0, inner, np.where(t < 2.0, outer, 0.0))


def weights(voxels, points, spacing):
    centre = (np.arange(points) - 2) * spacing + spacing / 2
    return spline((np.asarray(voxels)[:, None] + 0.5 - centre[None, :]) / spacing)


def halves(matrix):
    matrix = np.asarray(matrix, np.float32)
    high = matrix.astype(bf16)
    return high, (matrix - high.astype(np.float32)).astype(bf16)


def split(values):
    high = values.astype(bf16)
    return high, (values - high.astype(f32)).astype(bf16)


def mm(a, b):
    return jnp.dot(a, b, preferred_element_type=f32)


def mm3(values, high, low):
    a, b = split(values)
    return mm(a, high) + mm(b, high) + mm(a, low)


def lanes(shape):
    return lax.broadcasted_iota(jnp.int32, shape, len(shape) - 1)


def rows_of(shape):
    return lax.broadcasted_iota(jnp.int32, shape, len(shape) - 2)


def rolled(values, shift):
    shift %= values.shape[-1]
    return values if shift == 0 else pltpu.roll(values, shift, values.ndim - 1)


def within(mib):
    return pltpu.CompilerParams(vmem_limit_bytes=mib * 2**20)


def whole(n):
    return [pl.BlockSpec(memory_space=VMEM)] * n


PARTS = ((0, 4), (4, 12), (16, 16), (32, 16), (48, 16))


def faces_kernel(w_hbm, f_hbm, xf_ref, xo_ref, yf_ref, yo_ref, zf_ref, zo_ref, s_ref, t_ref, d_ref, w_ref, f_ref, sem):
    def copies(g):
        part = pl.ds(*PARTS[g])
        return [
            pltpu.make_async_copy(hbm.at[part], ref.at[part], sem.at[i, g])
            for i, (hbm, ref) in enumerate(((w_hbm, w_ref), (f_hbm, f_ref)))
        ]

    for g in range(len(PARTS)):
        for copy in copies(g):
            copy.start()
    lane = lanes((64, 128))
    for ref in (s_ref, t_ref):
        ref[:, 0:8, :] = jnp.zeros((68, 8, 128), f32)
        ref[:, 72:80, :] = jnp.zeros((68, 8, 128), f32)
        for x in (0, 1, 66, 67):
            ref[x, 8:72, :] = jnp.zeros((64, 128), f32)

    for g, (start, size) in enumerate(PARTS):
        for copy in copies(g):
            copy.wait()
        for x in range(start, start + size):
            w = w_ref[x]
            f = f_ref[x]
            s = w + f
            d = w - f
            s_ref[x + 2, 8:72, :] = s
            t_ref[x + 2, 8:72, :] = 8.0 * s
            d_ref[x] = d
            for j in range(2):
                yf_ref[j, x : x + 1, :] = s[62 + j : 63 + j]
                yf_ref[2 + j, x : x + 1, :] = d[62 + j : 63 + j]
                yo_ref[j, x : x + 1, :] = s[j : j + 1]
                yo_ref[2 + j, x : x + 1, :] = d[j : j + 1]
            i = x % 32
            here = (lane >= 4 * i) & (lane < 4 * i + 4)
            packed_s = rolled(s, 4 * i + 2) if i == 0 else jnp.where(here, rolled(s, 4 * i + 2), packed_s)
            packed_d = rolled(d, 4 * i + 2) if i == 0 else jnp.where(here, rolled(d, 4 * i + 2), packed_d)
            if i == 31:
                zo_ref[x // 32] = packed_s
                zo_ref[2 + x // 32] = packed_d

    for j in range(2):
        xf_ref[j] = s_ref[64 + j, 8:72, :]
        xf_ref[2 + j] = d_ref[62 + j]
        xo_ref[j] = s_ref[2 + j, 8:72, :]
        xo_ref[2 + j] = d_ref[j]
        zf_ref[j] = jnp.where(lane % 4 < 2, zo_ref[2 * j], rolled(zo_ref[2 * j + 1], 2))


def faces(w, f):
    shapes = [(4, 64, 128)] * 4 + [(2, 64, 128), (4, 64, 128)] + [(68, 80, 128)] * 2 + [(64, 64, 128)]
    return pl.pallas_call(
        faces_kernel,
        in_specs=[pl.BlockSpec(memory_space=pltpu.HBM)] * 2,
        out_specs=whole(9),
        out_shape=[jax.ShapeDtypeStruct(s, f32) for s in shapes],
        scratch_shapes=[
            VMEM((64, 64, 128), f32),
            VMEM((64, 64, 128), f32),
            pltpu.SemaphoreType.DMA((2, len(PARTS))),
        ],
        compiler_params=within(16),
        name="faces",
    )(*(pltpu.with_memory_space_constraint(v, pltpu.HBM) for v in (w, f)))


def bend_kernel(sizes, c_ref, k_ref, bf_ref, bk_ref, u_ref, k2_ref):
    nx, ny, nz = sizes
    ix, iy, iz = (lax.axis_index(n) for n in ("gx", "gy", "gz"))
    u_ref[...] = jnp.zeros_like(u_ref)
    for a in range(3):
        for p in range(8):
            at = 20 * (p + 2) + 2
            u_ref[a * 16 + 2 : a * 16 + 10, at : at + 16] = c_ref[a, p]
    lane = lanes((48, 256))
    row = rows_of((48, 256)) % 16
    gp = lane // 20 - 2 + 8 * ix
    gr = lane % 20 - 2 + 16 * iz
    gq = row - 2 + 8 * iy
    inside = (gp >= 0) & (gp < 8 * nx) & (gq >= 0) & (gq < 8 * ny) & (gr >= 0) & (gr < 16 * nz)

    def around(u, step):
        total = pltpu.roll(u, 1, 0) + pltpu.roll(u, u.shape[0] - 1, 0)
        for shift in (1, -1, step, -step):
            total = total + rolled(u, shift)
        return total - 6.0 * u

    u = around(u_ref[...], 20)
    u = around(jnp.where(inside, u, 0.0), 20) * BEND
    keep = lanes((48, 128)) < 120
    bf_ref[:, 0:128] = jnp.where(keep, u[:, 0:128], 0.0)
    bf_ref[:, 128:256] = jnp.where(keep, pltpu.roll(u, 136, 1)[:, 0:128], 0.0)

    kx, ky, kz = 2 * nx, 2 * ny, 4 * nz
    k2_ref[...] = jnp.zeros_like(k2_ref)
    parts = []
    for a in range(3):
        total = None
        for p in range(6):
            i = 6 * a + p
            k2_ref[i, 0:ky, 0:kz] = k_ref[a, jnp.clip(2 * ix - 2 + p, 0, kx - 1)]
            tile = pltpu.roll(k2_ref[i], (18 - 2 * iy) % 16, 0)[0:8]
            tile = pltpu.roll(tile, (130 - 4 * iz + 8 * p) % 128, 1)
            total = tile if p == 0 else jnp.where(lanes((8, 128)) // 8 == p, tile, total)
        parts.append(total)
    lane = lanes((24, 128))
    row = rows_of((24, 128)) % 8
    gp, gq, gr = 2 * ix - 2 + lane // 8, 2 * iy - 2 + row, 4 * iz - 2 + lane % 8
    inside = (gp >= 0) & (gp < kx) & (gq >= 0) & (gq < ky) & (gr >= 0) & (gr < kz) & (lane < 48)
    u = jnp.where(inside, jnp.concatenate(parts, 0), 0.0)
    u = around(jnp.where(inside, around(u, 8), 0.0), 8) * BEND
    own = (lane // 16 == 1) & (row // 2 == 1) & ((lane % 8 + 2) // 4 == 1)
    bk_ref[...] = rolled(jnp.where(own, u, 0.0), 80)


def bend(sizes, control, coarse):
    return pl.pallas_call(
        functools.partial(bend_kernel, sizes),
        in_specs=whole(2),
        out_specs=whole(2),
        out_shape=[
            jax.ShapeDtypeStruct((48, 256), f32),
            jax.ShapeDtypeStruct((24, 128), f32),
        ],
        scratch_shapes=[VMEM((48, 256), f32), VMEM((18, 16, 128), f32)],
        cost_estimate=pl.CostEstimate(flops=4000000, bytes_accessed=1000000, transcendentals=0),
        compiler_params=within(8),
        name="bend",
    )(control, coarse)


@functools.cache
def tables():
    own = np.arange(64)
    cross = np.arange(-2, 2)
    wy = np.zeros((24, 64))
    wy[0:12] = weights(own, 12, SPF).T
    wy[16:22] = weights(own, 6, SPC).T
    high, low = halves(wy)
    left = np.concatenate(
        [np.concatenate([high, high], 1), np.concatenate([low, np.zeros_like(low)], 1)], 0
    )
    wc = np.zeros((8, 8, 128), np.float32)
    for j in range(4):
        wc[j, :, :] = weights(cross, 12, SPF)[j, 0:8, None]
        wc[4 + j, 0:6, :] = weights(cross, 6, SPC)[j, :, None]
    fine_scale = SPF**-1.5 / 24.0
    coarse_scale = SPC**-1.5 / 24.0
    wz = np.zeros((2, 128, 128))
    wz[0, :, 0:20] = weights(np.arange(128), 20, SPF) * fine_scale
    wz[1, :, 0:8] = weights(np.arange(128), 8, SPC) * coarse_scale
    wz_high, wz_low = halves(wz)
    m = np.zeros((4, 128, 384))
    fx, cx = weights(own, 12, SPF), weights(own, 6, SPC)
    fz = weights(cross, 20, SPF) * fine_scale
    cz = weights(cross, 8, SPC) * coarse_scale
    fz = np.concatenate([fz, weights(np.arange(126, 128), 20, SPF) * fine_scale])
    cz = np.concatenate([cz, weights(np.arange(126, 128), 8, SPC) * coarse_scale])
    for x in range(64):
        for j in range(6):
            line = m[x // 32 + 2 * (j // 4), 4 * (x % 32) + j % 4]
            for p in range(12):
                at = 128 * (p // 6) + 20 * (p % 6)
                line[at : at + 20] = fx[x, p] * fz[j]
            for p in range(6):
                at = 256 + 80 + 8 * p
                line[at : at + 8] = cx[x, p] * cz[j]
    m_high, m_low = halves(m)
    return left, wc, wz_high, wz_low, m_high, m_low


def along(left, force):
    high, low = split(force)
    both = mm(left, jnp.concatenate([high, low], 0))
    return both[0:24] + both[24:48]


def interior_kernel(s_ref, t_ref, d_ref, left_ref, af_ref, ac_ref, tf_ref, tc_ref):
    fx = weights(np.arange(8), 5, SPF)
    cx = weights(np.arange(64), 6, SPC)
    left = left_ref[...]

    def force(x):
        d = d_ref[x]
        f0 = (s_ref[x, 8:72, :] - s_ref[x + 4, 8:72, :]) + (t_ref[x + 3, 8:72, :] - t_ref[x + 1, 8:72, :])
        s, t = s_ref.at[x + 2], t_ref.at[x + 2]
        f1 = (s[6:70, :] - s[10:74, :]) + (t[9:73, :] - t[7:71, :])
        s, t = s[8:72, :], t[8:72, :]
        f2 = (rolled(s, 2) - rolled(s, 126)) + (rolled(t, 127) - rolled(t, 1))
        return [f0 * d, f1 * d, f2 * d]

    def layers(b):
        for i in range(0, 8, 2):
            section = along(left, jnp.concatenate(force(8 * b + i) + force(8 * b + i + 1), 1))
            for k in range(6):
                at, a = 8 * b + i + k // 3, k % 3
                cols = slice(128 * k, 128 * k + 128)
                tf_ref[at, 16 * a : 16 * a + 16, :] = section[0:16, cols]
                tc_ref[at, 8 * a : 8 * a + 8, :] = section[16:24, cols]

    def block(b):
        for k in range(5):
            total = af_ref[b + k]
            for r in range(8):
                weight = float(fx[r, k])
                if weight != 0.0:
                    total = total + weight * tf_ref[8 * b + r]
            af_ref[b + k] = total
        for k in range((b + 2) // 4, (b + 2) // 4 + 4):
            total = ac_ref[k]
            for r in range(8):
                total = total + float(cx[8 * b + r, k]) * tc_ref[8 * b + r]
            ac_ref[k] = total

    af_ref[...] = jnp.zeros_like(af_ref)
    ac_ref[...] = jnp.zeros_like(ac_ref)
    for b in range(8):
        layers(b)
        if b > 0:
            block(b - 1)
    block(7)


def interior(s, s8, d):
    left = tables()[0]
    return pl.pallas_call(
        interior_kernel,
        in_specs=whole(4),
        out_specs=whole(2),
        out_shape=[
            jax.ShapeDtypeStruct((12, 48, 128), f32),
            jax.ShapeDtypeStruct((6, 24, 128), f32),
        ],
        scratch_shapes=[VMEM((64, 48, 128), f32), VMEM((64, 24, 128), f32)],
        cost_estimate=pl.CostEstimate(flops=40000000, bytes_accessed=4000000, transcendentals=0),
        compiler_params=within(16),
        name="interior",
    )(s, s8, d, jnp.asarray(left))


def crossing(first, second):
    sm2, sm1, dm2, dm1 = (first[i] for i in range(4))
    s0, s1, d0, d1 = (second[i] for i in range(4))
    return [-s0 * dm2, (8.0 * s0 - s1) * dm1, (sm2 - 8.0 * sm1) * d0, sm1 * d1]


def finish_kernel(
    af_ref, ac_ref, xr_ref, xo_ref, yr_ref, yo_ref, zr_ref, zo_ref, bf_ref, bk_ref, left_ref, wc_ref, wzh_ref, wzl_ref, mh_ref, ml_ref,
    chunk_ref, fine_ref, sf_ref, sc_ref,
):
    n = chunk_ref.shape[0]
    edge_f = weights(np.arange(-2, 2), 4, SPF)
    edge_c = weights(np.arange(-2, 2), 4, SPC)
    left = left_ref[...]
    lane = lanes((64, 128))

    edge = along(left, jnp.concatenate(crossing(xr_ref, xo_ref), 1))
    sf_ref[...] = af_ref[...]
    sc_ref[...] = ac_ref[...]
    for k in range(4):
        for j in range(4):
            cols = slice(128 * j, 128 * j + 128)
            fine = float(edge_f[j, k]) * edge[0:16, cols]
            coarse = float(edge_c[j, k]) * edge[16:24, cols]
            total_f = fine if j == 0 else total_f + fine
            total_c = coarse if j == 0 else total_c + coarse
        sf_ref[k, 0:16, :] += total_f
        sc_ref[k, 0:8, :] += total_c

    edge = along(left, jnp.concatenate(crossing(yr_ref, yo_ref), 1))
    for p in range(12):
        total = sf_ref[p, 16:24, :]
        for j in range(4):
            total = total + wc_ref[j] * edge[p : p + 1, 128 * j : 128 * j + 128]
        sf_ref[p, 16:24, :] = total
    for p in range(6):
        total = sc_ref[p, 8:16, :]
        for j in range(4):
            total = total + wc_ref[4 + j] * edge[16 + p : 17 + p, 128 * j : 128 * j + 128]
        sc_ref[p, 8:16, :] = total

    zf = mm3(sf_ref[...].reshape(576, 128), wzh_ref[0], wzl_ref[0])
    zc = mm3(sc_ref[...].reshape(144, 128), wzh_ref[1], wzl_ref[1])
    fine = []
    for h in range(2):
        total = zf[288 * h : 288 * h + 48]
        for i in range(1, 6):
            total = total + rolled(zf[48 * (6 * h + i) : 48 * (6 * h + i) + 48], 20 * i)
        fine.append(total + bf_ref[:, 128 * h : 128 * h + 128])
    coarse = bk_ref[...] + rolled(zc[0:24], 80)
    for p in range(1, 6):
        coarse = coarse + rolled(zc[24 * p : 24 * p + 24], 80 + 8 * p)

    j = lane % 4
    extra = None
    for h in range(2):
        s = jnp.where(j < 2, rolled(zr_ref[0], -2 * h) - zo_ref[h], zo_ref[h])
        d = jnp.where(j < 2, rolled(zr_ref[1], -2 * h), zo_ref[2 + h])
        slope = jnp.where(j >= 2, rolled(s, 2), 0.0) - jnp.where(j < 2, rolled(s, 126), 0.0)
        slope = slope + 8.0 * (
            jnp.where(j == 1, rolled(s, 127), 0.0) - jnp.where(j == 2, rolled(s, 1), 0.0)
        )
        wrapped = jnp.where(j < 2, -slope * zo_ref[2 + h], 0.0)
        part = along(left, jnp.concatenate([slope * d, wrapped], 1))
        part = mm3(part[:, 0:128], mh_ref[h], ml_ref[h]) + mm3(part[:, 128:256], mh_ref[2 + h], ml_ref[2 + h])
        extra = part if extra is None else extra + part

    zero8 = jnp.zeros((8, 128), f32)
    zero32 = jnp.zeros((32, 128), f32)
    low = fine[0] + jnp.concatenate([zero32, extra[0:16, 0:128]], 0)
    high = fine[1] + jnp.concatenate([zero32, extra[0:16, 128:256]], 0)
    spread = jnp.concatenate(
        [coarse[0:8], zero8, coarse[8:16], zero8, coarse[16:24] + extra[16:24, 256:384], zero8], 0
    )
    fine_ref[:, 0:128] = low
    fine_ref[:, 128:256] = high
    lane = lanes((48, 128))
    chunk = jnp.where(lane < 40, low, jnp.where(lane < 80, rolled(high, 88), spread))
    for i in range(n):
        for a in range(3):
            chunk_ref[i, 12 * a : 12 * a + 12, :] = chunk[16 * a : 16 * a + 12]
        chunk_ref[i, 36:40, :] = zero8[0:4]


def finish(n, *values):
    constants = tables()
    return pl.pallas_call(
        finish_kernel,
        in_specs=whole(16),
        out_specs=whole(2),
        out_shape=[
            jax.ShapeDtypeStruct((n, 40, 128), f32),
            jax.ShapeDtypeStruct((48, 256), f32),
        ],
        scratch_shapes=[VMEM((12, 48, 128), f32), VMEM((6, 24, 128), f32)],
        compiler_params=within(12),
        name="finish",
    )(*values, *(jnp.asarray(c) for c in constants))


def sides(ref, axis):
    n = ref.shape[0]
    i = lax.axis_index(axis)
    return ref[jnp.maximum(i - 1, 0)], i > 0, ref[jnp.minimum(i + 1, n - 1)], i < n - 1


def x_kernel(ny, got_ref, fine_ref, chunk_ref, own_ref, pack_ref):
    n = got_ref.shape[0]
    lane = lanes((24, 128))
    coarse = jnp.zeros((24, 128), f32)
    for j in range(n):
        part = jnp.concatenate([got_ref[j, 12 * a : 12 * a + 8, :] for a in range(3)], 0)
        first, last = max(0, 16 * j - 16), min(16 * n, 16 * j + 32)
        coarse = coarse + jnp.where((lane >= first) & (lane < last), rolled(part, 16 * j - 96), 0.0)
    low, has_low, high, has_high = sides(got_ref, "gx")
    lane = lanes((12, 128))
    middle = (lane >= 40) & (lane < 80)
    own_ref[...] = fine_ref[...]
    for a in range(3):
        rows = slice(16 * a, 16 * a + 12)
        own_ref[rows, 0:128] += jnp.where(middle & has_low, low[12 * a : 12 * a + 12], 0.0)
        own_ref[rows, 128:256] += jnp.where(middle & has_high, rolled(high[12 * a : 12 * a + 12], 40), 0.0)
    pack_ref[0:24, :] = coarse
    lane = lanes((2, 128))
    for m, q in ((0, 0), (2, 10)):
        last = jnp.zeros((2, 128), f32)
        for a in range(3):
            first = own_ref[16 * a + q : 16 * a + q + 2, 0:128]
            second = own_ref[16 * a + q : 16 * a + q + 2, 128:256]
            pack_ref[24 + 4 * a + m : 26 + 4 * a + m, :] = jnp.where(lane < 40, second, first)
            last = jnp.where((lane >= 40 * a) & (lane < 40 * a + 40), rolled(second, 40 * a - 40), last)
        pack_ref[36 + m : 38 + m, :] = last
    for i in range(ny):
        chunk_ref[i] = pack_ref[...]


def x_stage(ny, got, fine):
    return pl.pallas_call(
        functools.partial(x_kernel, ny),
        in_specs=whole(2),
        out_specs=whole(2),
        out_shape=[
            jax.ShapeDtypeStruct((ny, 40, 128), f32),
            jax.ShapeDtypeStruct((48, 256), f32),
        ],
        scratch_shapes=[VMEM((40, 128), f32)],
        compiler_params=within(4),
        name="xstage",
    )(got, fine)


def lane_of(p):
    return 128 * (p // 6), 20 * (p % 6)


def y_kernel(nz, got_ref, fine_ref, chunk_ref, own_ref, sum_ref):
    n = got_ref.shape[0]
    sum_ref[...] = jnp.zeros_like(sum_ref)
    for j in range(n):
        for a in range(3):
            at = 24 * a + 2 * j
            sum_ref[at : at + 6, :] += got_ref[j, 8 * a : 8 * a + 6, :]
    low, has_low, high, has_high = sides(got_ref, "gy")
    own_ref[...] = fine_ref[...]
    lane = lanes((2, 128))
    inner, tail = lane < 40, (lane >= 40) & (lane < 80)
    for a in range(3):
        for got, valid, m, q in ((low, has_low, 2, 2), (high, has_high, 0, 8)):
            rows = slice(16 * a + q, 16 * a + q + 2)
            first = got[24 + 4 * a + m : 26 + 4 * a + m]
            last = rolled(got[36 + m : 38 + m], 40 - 40 * a)
            second = jnp.where(inner, first, jnp.where(tail, last, 0.0))
            own_ref[rows, 0:128] += jnp.where(valid & ~inner, first, 0.0)
            own_ref[rows, 128:256] += jnp.where(valid, second, 0.0)
    lane = lanes((8, 128))
    border = jnp.zeros((8, 128), f32)
    for a in range(3):
        for p in range(8):
            tile, base = lane_of(p + 2)
            v = own_ref[16 * a + 2 : 16 * a + 10, tile : tile + 128]
            at = 32 * a + 4 * p
            border = jnp.where((lane >= at) & (lane < at + 2), rolled(v, at - base), border)
            border = jnp.where((lane >= at + 2) & (lane < at + 4), rolled(v, at - base - 16), border)
    for i in range(nz):
        for a in range(3):
            chunk_ref[i, 16 * a : 16 * a + 16, :] = sum_ref[24 * a + 2 : 24 * a + 18, :]
        chunk_ref[i, 48:56, :] = border


def y_stage(nz, got, fine):
    return pl.pallas_call(
        functools.partial(y_kernel, nz),
        in_specs=whole(2),
        out_specs=whole(2),
        out_shape=[
            jax.ShapeDtypeStruct((nz, 56, 128), f32),
            jax.ShapeDtypeStruct((48, 256), f32),
        ],
        scratch_shapes=[VMEM((72, 128), f32)],
        compiler_params=within(4),
        name="ystage",
    )(got, fine)


def z_kernel(nx, ny, got_ref, fine_ref, out_fine_ref, out_coarse_ref):
    n = got_ref.shape[0]
    low, has_low, high, has_high = sides(got_ref, "gz")
    low = jnp.where(has_low, low[48:56], 0.0)
    high = jnp.where(has_high, high[48:56], 0.0)
    lane = lanes((8, 128))
    for a in range(3):
        for p in range(8):
            tile, base = lane_of(p + 2)
            v = fine_ref[16 * a + 2 : 16 * a + 10, tile : tile + 128]
            at = 32 * a + 4 * p
            v = v + jnp.where((lane >= base + 2) & (lane < base + 4), rolled(low, base - at), 0.0)
            v = v + jnp.where((lane >= base + 16) & (lane < base + 18), rolled(high, base + 16 - at), 0.0)
            out_fine_ref[a, p] = rolled(v, -(base + 2))[:, 0:16]

    lane = lanes((48, 128))
    k = lane % 8
    parts = [got_ref[m, 0:48, :] for m in range(n)]
    tiles = []
    for m in range(0, n, 2):
        total = jnp.where(k < 6, rolled(parts[m], -2), 0.0) + jnp.where(k >= 2, rolled(parts[m + 1], 2), 0.0)
        if m > 0:
            total = total + jnp.where(k < 2, rolled(parts[m - 1], -6), 0.0)
        if m + 2 < n:
            total = total + jnp.where(k >= 6, rolled(parts[m + 2], 6), 0.0)
        tiles.append(total)
    per = len(tiles)
    slot = lane // 8 % per
    for h in range(per):
        total = rolled(tiles[0], -8 * h)
        for m in range(1, per):
            total = jnp.where(slot == m, rolled(tiles[m], 8 * (m - h)), total)
        for g in range(2 * nx // per):
            points = rolled(total, -8 * per * g)
            for a in range(3):
                out_coarse_ref[a, per * g + h] = points[16 * a : 16 * a + 2 * ny, 0 : 4 * n]


def z_stage(sizes, got, fine):
    nx, ny, nz = sizes
    return pl.pallas_call(
        functools.partial(z_kernel, nx, ny),
        in_specs=whole(2),
        out_specs=whole(2),
        out_shape=[
            jax.ShapeDtypeStruct((3, 8, 8, 16), f32),
            jax.ShapeDtypeStruct((3, 2 * nx, 2 * ny, 4 * nz), f32),
        ],
        compiler_params=within(6),
        name="zstage",
    )(got, fine)


def shifted_up(values, axis):
    return lax.ppermute(values, axis, [(i, i + 1) for i in range(lax.axis_size(axis) - 1)])


def exchanged(chunks, axis):
    return lax.all_to_all(chunks, axis, split_axis=0, concat_axis=0, tiled=True)


def per_device(warped_image, fixed_image, fine_control, coarse_control):
    sizes = tuple(lax.axis_size(n) for n in ("gx", "gy", "gz"))
    xf, xo, yf, yo, zf, zo, s, s8, d = faces(warped_image, fixed_image)
    yr = shifted_up(yf, "gy")
    zr = shifted_up(zf, "gz")
    xr = shifted_up(xf, "gx")
    bent_fine, bent_coarse = bend(sizes, fine_control, coarse_control)
    fine, coarse = interior(s, s8, d)
    chunk, fine = finish(sizes[0], fine, coarse, xr, xo, yr, yo, zr, zo, bent_fine, bent_coarse)
    chunk, fine = x_stage(sizes[1], exchanged(chunk, "gx"), fine)
    chunk, fine = y_stage(sizes[2], exchanged(chunk, "gy"), fine)
    return tuple(z_stage(sizes, exchanged(chunk, "gz"), fine))


def solution(mesh):
    in_specs = (P("gx", "gy", "gz"), P("gx", "gy", "gz"), P(None, "gx", "gy", "gz"), P())
    out_specs = (P(None, "gx", "gy", "gz"), P())
    return jax.shard_map(
        per_device, mesh=mesh, in_specs=in_specs, out_specs=out_specs, check_vma=False
    )
```

```python
import functools

import jax
import jax.numpy as jnp
import numpy as np
from jax import lax
from jax.experimental import pallas as pl
from jax.experimental.pallas import tpu as pltpu
from jax.sharding import PartitionSpec as P

SPF = 8
SPC = 32
BEND = 0.01
f32 = jnp.float32
bf16 = jnp.bfloat16
VMEM = pltpu.VMEM


def spline(t):
    t = np.abs(t)
    inner = 2.0 / 3.0 - t * t + 0.5 * t**3
    outer = (2.0 - t) ** 3 / 6.0
    return np.where(t < 1.0, inner, np.where(t < 2.0, outer, 0.0))


def weights(voxels, points, spacing):
    centre = (np.arange(points) - 2) * spacing + spacing / 2
    return spline((np.asarray(voxels)[:, None] + 0.5 - centre[None, :]) / spacing)


def halves(matrix):
    matrix = np.asarray(matrix, np.float32)
    high = matrix.astype(bf16)
    return high, (matrix - high.astype(np.float32)).astype(bf16)


def split(values):
    high = values.astype(bf16)
    return high, (values - high.astype(f32)).astype(bf16)


def mm(a, b):
    return jnp.dot(a, b, preferred_element_type=f32)


def mm3(values, high, low):
    a, b = split(values)
    return mm(a, high) + mm(b, high) + mm(a, low)


def lanes(shape):
    return lax.broadcasted_iota(jnp.int32, shape, len(shape) - 1)


def rows_of(shape):
    return lax.broadcasted_iota(jnp.int32, shape, len(shape) - 2)


def rolled(values, shift):
    shift %= values.shape[-1]
    return values if shift == 0 else pltpu.roll(values, shift, values.ndim - 1)


def within(mib):
    return pltpu.CompilerParams(vmem_limit_bytes=mib * 2**20)


def whole(n):
    return [pl.BlockSpec(memory_space=VMEM)] * n


def edges_kernel(w_hbm, f_hbm, xf_ref, yf_ref, px_ref, py_ref, sem):
    copies = []
    for i, hbm in enumerate((w_hbm, f_hbm)):
        copies.append(pltpu.make_async_copy(hbm.at[:, pl.ds(56, 8)], py_ref.at[i], sem.at[0, i]))
        copies.append(pltpu.make_async_copy(hbm.at[pl.ds(62, 2)], px_ref.at[i], sem.at[1, i]))
    for copy in copies:
        copy.start()
    for copy in copies:
        copy.wait()
    for x in range(64):
        w, f = py_ref[0, x], py_ref[1, x]
        s, d = w + f, w - f
        for j in range(2):
            yf_ref[j, x : x + 1, :] = s[6 + j : 7 + j]
            yf_ref[2 + j, x : x + 1, :] = d[6 + j : 7 + j]
    xf_ref[0:2] = px_ref[0] + px_ref[1]
    xf_ref[2:4] = px_ref[0] - px_ref[1]


def edges(w, f):
    return pl.pallas_call(
        edges_kernel,
        in_specs=[pl.BlockSpec(memory_space=pltpu.HBM)] * 2,
        out_specs=whole(2),
        out_shape=[jax.ShapeDtypeStruct((4, 64, 128), f32)] * 2,
        scratch_shapes=[
            VMEM((2, 2, 64, 128), f32),
            VMEM((2, 64, 8, 128), f32),
            pltpu.SemaphoreType.DMA((2, 2)),
        ],
        cost_estimate=pl.CostEstimate(flops=1000000, bytes_accessed=1000000, transcendentals=0),
        compiler_params=within(4),
        name="edges",
    )(*(pltpu.with_memory_space_constraint(v, pltpu.HBM) for v in (w, f)))


def faces_kernel(w_ref, f_ref, xo_ref, yo_ref, zf_ref, zo_ref, s_ref, t_ref, d_ref):
    lane = lanes((64, 128))
    for ref in (s_ref, t_ref):
        ref[:, 0:8, :] = jnp.zeros((68, 8, 128), f32)
        ref[:, 72:80, :] = jnp.zeros((68, 8, 128), f32)
        for x in (0, 1, 66, 67):
            ref[x, 8:72, :] = jnp.zeros((64, 128), f32)

    for x in range(64):
        w = w_ref[x]
        f = f_ref[x]
        s = w + f
        d = w - f
        s_ref[x + 2, 8:72, :] = s
        t_ref[x + 2, 8:72, :] = 8.0 * s
        d_ref[x] = d
        for j in range(2):
            yo_ref[j, x : x + 1, :] = s[j : j + 1]
            yo_ref[2 + j, x : x + 1, :] = d[j : j + 1]
        i = x % 32
        here = (lane >= 4 * i) & (lane < 4 * i + 4)
        packed_s = rolled(s, 4 * i + 2) if i == 0 else jnp.where(here, rolled(s, 4 * i + 2), packed_s)
        packed_d = rolled(d, 4 * i + 2) if i == 0 else jnp.where(here, rolled(d, 4 * i + 2), packed_d)
        if i == 31:
            zo_ref[x // 32] = packed_s
            zo_ref[2 + x // 32] = packed_d

    for j in range(2):
        xo_ref[j] = s_ref[2 + j, 8:72, :]
        xo_ref[2 + j] = d_ref[j]
        zf_ref[j] = jnp.where(lane % 4 < 2, zo_ref[2 * j], rolled(zo_ref[2 * j + 1], 2))


def faces(w, f):
    shapes = [(4, 64, 128)] * 2 + [(2, 64, 128), (4, 64, 128)] + [(68, 80, 128)] * 2 + [(64, 64, 128)]
    return pl.pallas_call(
        faces_kernel,
        in_specs=whole(2),
        out_specs=whole(7),
        out_shape=[jax.ShapeDtypeStruct(s, f32) for s in shapes],
        cost_estimate=pl.CostEstimate(flops=20000000, bytes_accessed=4000000, transcendentals=0),
        compiler_params=within(4),
        name="faces",
    )(w, f)


def bend_kernel(sizes, c_ref, k_ref, bf_ref, bk_ref, u_ref, k2_ref):
    nx, ny, nz = sizes
    ix, iy, iz = (lax.axis_index(n) for n in ("gx", "gy", "gz"))
    u_ref[...] = jnp.zeros_like(u_ref)
    for a in range(3):
        for p in range(8):
            at = 20 * (p + 2) + 2
            u_ref[a * 16 + 2 : a * 16 + 10, at : at + 16] = c_ref[a, p]
    lane = lanes((48, 256))
    row = rows_of((48, 256)) % 16
    gp = lane // 20 - 2 + 8 * ix
    gr = lane % 20 - 2 + 16 * iz
    gq = row - 2 + 8 * iy
    inside = (gp >= 0) & (gp < 8 * nx) & (gq >= 0) & (gq < 8 * ny) & (gr >= 0) & (gr < 16 * nz)

    def around(u, step):
        total = pltpu.roll(u, 1, 0) + pltpu.roll(u, u.shape[0] - 1, 0)
        for shift in (1, -1, step, -step):
            total = total + rolled(u, shift)
        return total - 6.0 * u

    u = around(u_ref[...], 20)
    u = around(jnp.where(inside, u, 0.0), 20) * BEND
    keep = lanes((48, 128)) < 120
    bf_ref[:, 0:128] = jnp.where(keep, u[:, 0:128], 0.0)
    bf_ref[:, 128:256] = jnp.where(keep, pltpu.roll(u, 136, 1)[:, 0:128], 0.0)

    kx, ky, kz = 2 * nx, 2 * ny, 4 * nz
    k2_ref[...] = jnp.zeros_like(k2_ref)
    parts = []
    for a in range(3):
        total = None
        for p in range(6):
            i = 6 * a + p
            k2_ref[i, 0:ky, 0:kz] = k_ref[a, jnp.clip(2 * ix - 2 + p, 0, kx - 1)]
            tile = pltpu.roll(k2_ref[i], (18 - 2 * iy) % 16, 0)[0:8]
            tile = pltpu.roll(tile, (130 - 4 * iz + 8 * p) % 128, 1)
            total = tile if p == 0 else jnp.where(lanes((8, 128)) // 8 == p, tile, total)
        parts.append(total)
    lane = lanes((24, 128))
    row = rows_of((24, 128)) % 8
    gp, gq, gr = 2 * ix - 2 + lane // 8, 2 * iy - 2 + row, 4 * iz - 2 + lane % 8
    inside = (gp >= 0) & (gp < kx) & (gq >= 0) & (gq < ky) & (gr >= 0) & (gr < kz) & (lane < 48)
    u = jnp.where(inside, jnp.concatenate(parts, 0), 0.0)
    u = around(jnp.where(inside, around(u, 8), 0.0), 8) * BEND
    own = (lane // 16 == 1) & (row // 2 == 1) & ((lane % 8 + 2) // 4 == 1)
    bk_ref[...] = rolled(jnp.where(own, u, 0.0), 80)


def bend(sizes, control, coarse):
    return pl.pallas_call(
        functools.partial(bend_kernel, sizes),
        in_specs=whole(2),
        out_specs=whole(2),
        out_shape=[
            jax.ShapeDtypeStruct((48, 256), f32),
            jax.ShapeDtypeStruct((24, 128), f32),
        ],
        scratch_shapes=[VMEM((48, 256), f32), VMEM((18, 16, 128), f32)],
        cost_estimate=pl.CostEstimate(flops=4000000, bytes_accessed=1000000, transcendentals=0),
        compiler_params=within(8),
        name="bend",
    )(control, coarse)


@functools.cache
def tables():
    own = np.arange(64)
    cross = np.arange(-2, 2)
    wy = np.zeros((24, 64))
    wy[0:12] = weights(own, 12, SPF).T
    wy[16:22] = weights(own, 6, SPC).T
    high, low = halves(wy)
    left = np.concatenate(
        [np.concatenate([high, high], 1), np.concatenate([low, np.zeros_like(low)], 1)], 0
    )
    wc = np.zeros((8, 8, 128), np.float32)
    for j in range(4):
        wc[j, :, :] = weights(cross, 12, SPF)[j, 0:8, None]
        wc[4 + j, 0:6, :] = weights(cross, 6, SPC)[j, :, None]
    fine_scale = SPF**-1.5 / 24.0
    coarse_scale = SPC**-1.5 / 24.0
    wz = np.zeros((2, 128, 128))
    wz[0, :, 0:20] = weights(np.arange(128), 20, SPF) * fine_scale
    wz[1, :, 0:8] = weights(np.arange(128), 8, SPC) * coarse_scale
    wz_high, wz_low = halves(wz)
    m = np.zeros((4, 128, 384))
    fx, cx = weights(own, 12, SPF), weights(own, 6, SPC)
    fz = weights(cross, 20, SPF) * fine_scale
    cz = weights(cross, 8, SPC) * coarse_scale
    fz = np.concatenate([fz, weights(np.arange(126, 128), 20, SPF) * fine_scale])
    cz = np.concatenate([cz, weights(np.arange(126, 128), 8, SPC) * coarse_scale])
    for x in range(64):
        for j in range(6):
            line = m[x // 32 + 2 * (j // 4), 4 * (x % 32) + j % 4]
            for p in range(12):
                at = 128 * (p // 6) + 20 * (p % 6)
                line[at : at + 20] = fx[x, p] * fz[j]
            for p in range(6):
                at = 256 + 80 + 8 * p
                line[at : at + 8] = cx[x, p] * cz[j]
    m_high, m_low = halves(m)
    return left, wc, wz_high, wz_low, m_high, m_low


def along(left, force):
    high, low = split(force)
    both = mm(left, jnp.concatenate([high, low], 0))
    return both[0:24] + both[24:48]


def interior_kernel(s_ref, t_ref, d_ref, left_ref, af_ref, ac_ref, tf_ref, tc_ref):
    fx = weights(np.arange(8), 5, SPF)
    cx = weights(np.arange(64), 6, SPC)
    left = left_ref[...]

    def force(x):
        d = d_ref[x]
        f0 = (s_ref[x, 8:72, :] - s_ref[x + 4, 8:72, :]) + (t_ref[x + 3, 8:72, :] - t_ref[x + 1, 8:72, :])
        s, t = s_ref.at[x + 2], t_ref.at[x + 2]
        f1 = (s[6:70, :] - s[10:74, :]) + (t[9:73, :] - t[7:71, :])
        s, t = s[8:72, :], t[8:72, :]
        f2 = (rolled(s, 2) - rolled(s, 126)) + (rolled(t, 127) - rolled(t, 1))
        return [f0 * d, f1 * d, f2 * d]

    def layers(b):
        for i in range(0, 8, 2):
            section = along(left, jnp.concatenate(force(8 * b + i) + force(8 * b + i + 1), 1))
            for k in range(6):
                at, a = 8 * b + i + k // 3, k % 3
                cols = slice(128 * k, 128 * k + 128)
                tf_ref[at, 16 * a : 16 * a + 16, :] = section[0:16, cols]
                tc_ref[at, 8 * a : 8 * a + 8, :] = section[16:24, cols]

    def block(b):
        for k in range(5):
            total = af_ref[b + k]
            for r in range(8):
                weight = float(fx[r, k])
                if weight != 0.0:
                    total = total + weight * tf_ref[8 * b + r]
            af_ref[b + k] = total
        for k in range((b + 2) // 4, (b + 2) // 4 + 4):
            total = ac_ref[k]
            for r in range(8):
                total = total + float(cx[8 * b + r, k]) * tc_ref[8 * b + r]
            ac_ref[k] = total

    af_ref[...] = jnp.zeros_like(af_ref)
    ac_ref[...] = jnp.zeros_like(ac_ref)
    for b in range(8):
        layers(b)
        if b > 0:
            block(b - 1)
    block(7)


def interior(s, s8, d):
    left = tables()[0]
    return pl.pallas_call(
        interior_kernel,
        in_specs=whole(4),
        out_specs=whole(2),
        out_shape=[
            jax.ShapeDtypeStruct((12, 48, 128), f32),
            jax.ShapeDtypeStruct((6, 24, 128), f32),
        ],
        scratch_shapes=[VMEM((64, 48, 128), f32), VMEM((64, 24, 128), f32)],
        cost_estimate=pl.CostEstimate(flops=40000000, bytes_accessed=4000000, transcendentals=0),
        compiler_params=within(16),
        name="interior",
    )(s, s8, d, jnp.asarray(left))


def crossing(first, second):
    sm2, sm1, dm2, dm1 = (first[i] for i in range(4))
    s0, s1, d0, d1 = (second[i] for i in range(4))
    return [-s0 * dm2, (8.0 * s0 - s1) * dm1, (sm2 - 8.0 * sm1) * d0, sm1 * d1]


def finish_kernel(
    af_ref, ac_ref, xr_ref, xo_ref, yr_ref, yo_ref, zr_ref, zo_ref, bf_ref, bk_ref, left_ref, wc_ref, wzh_ref, wzl_ref, mh_ref, ml_ref,
    chunk_ref, fine_ref, sf_ref, sc_ref,
):
    n = chunk_ref.shape[0]
    edge_f = weights(np.arange(-2, 2), 4, SPF)
    edge_c = weights(np.arange(-2, 2), 4, SPC)
    left = left_ref[...]
    lane = lanes((64, 128))

    edge = along(left, jnp.concatenate(crossing(xr_ref, xo_ref), 1))
    sf_ref[...] = af_ref[...]
    sc_ref[...] = ac_ref[...]
    for k in range(4):
        for j in range(4):
            cols = slice(128 * j, 128 * j + 128)
            fine = float(edge_f[j, k]) * edge[0:16, cols]
            coarse = float(edge_c[j, k]) * edge[16:24, cols]
            total_f = fine if j == 0 else total_f + fine
            total_c = coarse if j == 0 else total_c + coarse
        sf_ref[k, 0:16, :] += total_f
        sc_ref[k, 0:8, :] += total_c

    edge = along(left, jnp.concatenate(crossing(yr_ref, yo_ref), 1))
    for p in range(12):
        total = sf_ref[p, 16:24, :]
        for j in range(4):
            total = total + wc_ref[j] * edge[p : p + 1, 128 * j : 128 * j + 128]
        sf_ref[p, 16:24, :] = total
    for p in range(6):
        total = sc_ref[p, 8:16, :]
        for j in range(4):
            total = total + wc_ref[4 + j] * edge[16 + p : 17 + p, 128 * j : 128 * j + 128]
        sc_ref[p, 8:16, :] = total

    zf = mm3(sf_ref[...].reshape(576, 128), wzh_ref[0], wzl_ref[0])
    zc = mm3(sc_ref[...].reshape(144, 128), wzh_ref[1], wzl_ref[1])
    fine = []
    for h in range(2):
        total = zf[288 * h : 288 * h + 48]
        for i in range(1, 6):
            total = total + rolled(zf[48 * (6 * h + i) : 48 * (6 * h + i) + 48], 20 * i)
        fine.append(total + bf_ref[:, 128 * h : 128 * h + 128])
    coarse = bk_ref[...] + rolled(zc[0:24], 80)
    for p in range(1, 6):
        coarse = coarse + rolled(zc[24 * p : 24 * p + 24], 80 + 8 * p)

    j = lane % 4
    extra = None
    for h in range(2):
        s = jnp.where(j < 2, rolled(zr_ref[0], -2 * h) - zo_ref[h], zo_ref[h])
        d = jnp.where(j < 2, rolled(zr_ref[1], -2 * h), zo_ref[2 + h])
        slope = jnp.where(j >= 2, rolled(s, 2), 0.0) - jnp.where(j < 2, rolled(s, 126), 0.0)
        slope = slope + 8.0 * (
            jnp.where(j == 1, rolled(s, 127), 0.0) - jnp.where(j == 2, rolled(s, 1), 0.0)
        )
        wrapped = jnp.where(j < 2, -slope * zo_ref[2 + h], 0.0)
        part = along(left, jnp.concatenate([slope * d, wrapped], 1))
        part = mm3(part[:, 0:128], mh_ref[h], ml_ref[h]) + mm3(part[:, 128:256], mh_ref[2 + h], ml_ref[2 + h])
        extra = part if extra is None else extra + part

    zero8 = jnp.zeros((8, 128), f32)
    zero32 = jnp.zeros((32, 128), f32)
    low = fine[0] + jnp.concatenate([zero32, extra[0:16, 0:128]], 0)
    high = fine[1] + jnp.concatenate([zero32, extra[0:16, 128:256]], 0)
    spread = jnp.concatenate(
        [coarse[0:8], zero8, coarse[8:16], zero8, coarse[16:24] + extra[16:24, 256:384], zero8], 0
    )
    fine_ref[:, 0:128] = low
    fine_ref[:, 128:256] = high
    lane = lanes((48, 128))
    chunk = jnp.where(lane < 40, low, jnp.where(lane < 80, rolled(high, 88), spread))
    for i in range(n):
        for a in range(3):
            chunk_ref[i, 12 * a : 12 * a + 12, :] = chunk[16 * a : 16 * a + 12]
        chunk_ref[i, 36:40, :] = zero8[0:4]


def finish(n, *values):
    constants = tables()
    return pl.pallas_call(
        finish_kernel,
        in_specs=whole(16),
        out_specs=whole(2),
        out_shape=[
            jax.ShapeDtypeStruct((n, 40, 128), f32),
            jax.ShapeDtypeStruct((48, 256), f32),
        ],
        scratch_shapes=[VMEM((12, 48, 128), f32), VMEM((6, 24, 128), f32)],
        compiler_params=within(12),
        name="finish",
    )(*values, *(jnp.asarray(c) for c in constants))


def sides(ref, axis):
    n = ref.shape[0]
    i = lax.axis_index(axis)
    return ref[jnp.maximum(i - 1, 0)], i > 0, ref[jnp.minimum(i + 1, n - 1)], i < n - 1


def x_kernel(ny, got_ref, fine_ref, chunk_ref, own_ref, pack_ref):
    n = got_ref.shape[0]
    lane = lanes((24, 128))
    coarse = jnp.zeros((24, 128), f32)
    for j in range(n):
        part = jnp.concatenate([got_ref[j, 12 * a : 12 * a + 8, :] for a in range(3)], 0)
        first, last = max(0, 16 * j - 16), min(16 * n, 16 * j + 32)
        coarse = coarse + jnp.where((lane >= first) & (lane < last), rolled(part, 16 * j - 96), 0.0)
    low, has_low, high, has_high = sides(got_ref, "gx")
    lane = lanes((12, 128))
    middle = (lane >= 40) & (lane < 80)
    own_ref[...] = fine_ref[...]
    for a in range(3):
        rows = slice(16 * a, 16 * a + 12)
        own_ref[rows, 0:128] += jnp.where(middle & has_low, low[12 * a : 12 * a + 12], 0.0)
        own_ref[rows, 128:256] += jnp.where(middle & has_high, rolled(high[12 * a : 12 * a + 12], 40), 0.0)
    pack_ref[0:24, :] = coarse
    lane = lanes((2, 128))
    for m, q in ((0, 0), (2, 10)):
        last = jnp.zeros((2, 128), f32)
        for a in range(3):
            first = own_ref[16 * a + q : 16 * a + q + 2, 0:128]
            second = own_ref[16 * a + q : 16 * a + q + 2, 128:256]
            pack_ref[24 + 4 * a + m : 26 + 4 * a + m, :] = jnp.where(lane < 40, second, first)
            last = jnp.where((lane >= 40 * a) & (lane < 40 * a + 40), rolled(second, 40 * a - 40), last)
        pack_ref[36 + m : 38 + m, :] = last
    for i in range(ny):
        chunk_ref[i] = pack_ref[...]


def x_stage(ny, got, fine):
    return pl.pallas_call(
        functools.partial(x_kernel, ny),
        in_specs=whole(2),
        out_specs=whole(2),
        out_shape=[
            jax.ShapeDtypeStruct((ny, 40, 128), f32),
            jax.ShapeDtypeStruct((48, 256), f32),
        ],
        scratch_shapes=[VMEM((40, 128), f32)],
        compiler_params=within(4),
        name="xstage",
    )(got, fine)


def lane_of(p):
    return 128 * (p // 6), 20 * (p % 6)


def y_kernel(nz, got_ref, fine_ref, chunk_ref, own_ref, sum_ref):
    n = got_ref.shape[0]
    sum_ref[...] = jnp.zeros_like(sum_ref)
    for j in range(n):
        for a in range(3):
            at = 24 * a + 2 * j
            sum_ref[at : at + 6, :] += got_ref[j, 8 * a : 8 * a + 6, :]
    low, has_low, high, has_high = sides(got_ref, "gy")
    own_ref[...] = fine_ref[...]
    lane = lanes((2, 128))
    inner, tail = lane < 40, (lane >= 40) & (lane < 80)
    for a in range(3):
        for got, valid, m, q in ((low, has_low, 2, 2), (high, has_high, 0, 8)):
            rows = slice(16 * a + q, 16 * a + q + 2)
            first = got[24 + 4 * a + m : 26 + 4 * a + m]
            last = rolled(got[36 + m : 38 + m], 40 - 40 * a)
            second = jnp.where(inner, first, jnp.where(tail, last, 0.0))
            own_ref[rows, 0:128] += jnp.where(valid & ~inner, first, 0.0)
            own_ref[rows, 128:256] += jnp.where(valid, second, 0.0)
    lane = lanes((8, 128))
    border = jnp.zeros((8, 128), f32)
    for a in range(3):
        for p in range(8):
            tile, base = lane_of(p + 2)
            v = own_ref[16 * a + 2 : 16 * a + 10, tile : tile + 128]
            at = 32 * a + 4 * p
            border = jnp.where((lane >= at) & (lane < at + 2), rolled(v, at - base), border)
            border = jnp.where((lane >= at + 2) & (lane < at + 4), rolled(v, at - base - 16), border)
    for i in range(nz):
        for a in range(3):
            chunk_ref[i, 16 * a : 16 * a + 16, :] = sum_ref[24 * a + 2 : 24 * a + 18, :]
        chunk_ref[i, 48:56, :] = border


def y_stage(nz, got, fine):
    return pl.pallas_call(
        functools.partial(y_kernel, nz),
        in_specs=whole(2),
        out_specs=whole(2),
        out_shape=[
            jax.ShapeDtypeStruct((nz, 56, 128), f32),
            jax.ShapeDtypeStruct((48, 256), f32),
        ],
        scratch_shapes=[VMEM((72, 128), f32)],
        compiler_params=within(4),
        name="ystage",
    )(got, fine)


def z_kernel(nx, ny, got_ref, fine_ref, out_fine_ref, out_coarse_ref):
    n = got_ref.shape[0]
    low, has_low, high, has_high = sides(got_ref, "gz")
    low = jnp.where(has_low, low[48:56], 0.0)
    high = jnp.where(has_high, high[48:56], 0.0)
    lane = lanes((8, 128))
    for a in range(3):
        for p in range(8):
            tile, base = lane_of(p + 2)
            v = fine_ref[16 * a + 2 : 16 * a + 10, tile : tile + 128]
            at = 32 * a + 4 * p
            v = v + jnp.where((lane >= base + 2) & (lane < base + 4), rolled(low, base - at), 0.0)
            v = v + jnp.where((lane >= base + 16) & (lane < base + 18), rolled(high, base + 16 - at), 0.0)
            out_fine_ref[a, p] = rolled(v, -(base + 2))[:, 0:16]

    lane = lanes((48, 128))
    k = lane % 8
    parts = [got_ref[m, 0:48, :] for m in range(n)]
    tiles = []
    for m in range(0, n, 2):
        total = jnp.where(k < 6, rolled(parts[m], -2), 0.0) + jnp.where(k >= 2, rolled(parts[m + 1], 2), 0.0)
        if m > 0:
            total = total + jnp.where(k < 2, rolled(parts[m - 1], -6), 0.0)
        if m + 2 < n:
            total = total + jnp.where(k >= 6, rolled(parts[m + 2], 6), 0.0)
        tiles.append(total)
    per = len(tiles)
    slot = lane // 8 % per
    for h in range(per):
        total = rolled(tiles[0], -8 * h)
        for m in range(1, per):
            total = jnp.where(slot == m, rolled(tiles[m], 8 * (m - h)), total)
        for g in range(2 * nx // per):
            points = rolled(total, -8 * per * g)
            for a in range(3):
                out_coarse_ref[a, per * g + h] = points[16 * a : 16 * a + 2 * ny, 0 : 4 * n]


def z_stage(sizes, got, fine):
    nx, ny, nz = sizes
    return pl.pallas_call(
        functools.partial(z_kernel, nx, ny),
        in_specs=whole(2),
        out_specs=whole(2),
        out_shape=[
            jax.ShapeDtypeStruct((3, 8, 8, 16), f32),
            jax.ShapeDtypeStruct((3, 2 * nx, 2 * ny, 4 * nz), f32),
        ],
        compiler_params=within(6),
        name="zstage",
    )(got, fine)


def shifted_up(values, axis):
    return lax.ppermute(values, axis, [(i, i + 1) for i in range(lax.axis_size(axis) - 1)])


def exchanged(chunks, axis):
    return lax.all_to_all(chunks, axis, split_axis=0, concat_axis=0, tiled=True)


def per_device(warped_image, fixed_image, fine_control, coarse_control):
    sizes = tuple(lax.axis_size(n) for n in ("gx", "gy", "gz"))
    xf, yf = edges(warped_image, fixed_image)
    yr = shifted_up(yf, "gy")
    xr = shifted_up(xf, "gx")
    xo, yo, zf, zo, s, s8, d = faces(warped_image, fixed_image)
    zr = shifted_up(zf, "gz")
    bent_fine, bent_coarse = bend(sizes, fine_control, coarse_control)
    fine, coarse = interior(s, s8, d)
    chunk, fine = finish(sizes[0], fine, coarse, xr, xo, yr, yo, zr, zo, bent_fine, bent_coarse)
    chunk, fine = x_stage(sizes[1], exchanged(chunk, "gx"), fine)
    chunk, fine = y_stage(sizes[2], exchanged(chunk, "gy"), fine)
    return tuple(z_stage(sizes, exchanged(chunk, "gz"), fine))


def solution(mesh):
    in_specs = (P("gx", "gy", "gz"), P("gx", "gy", "gz"), P(None, "gx", "gy", "gz"), P())
    out_specs = (P(None, "gx", "gy", "gz"), P())
    return jax.shard_map(
        per_device, mesh=mesh, in_specs=in_specs, out_specs=out_specs, check_vma=False
    )
```

```python
import functools

import jax
import jax.numpy as jnp
import numpy as np
from jax import lax
from jax.experimental import pallas as pl
from jax.experimental.pallas import tpu as pltpu
from jax.sharding import PartitionSpec as P

SPF = 8
SPC = 32
BEND = 0.01
f32 = jnp.float32
bf16 = jnp.bfloat16
VMEM = pltpu.VMEM


def spline(t):
    t = np.abs(t)
    inner = 2.0 / 3.0 - t * t + 0.5 * t**3
    outer = (2.0 - t) ** 3 / 6.0
    return np.where(t < 1.0, inner, np.where(t < 2.0, outer, 0.0))


def weights(voxels, points, spacing):
    centre = (np.arange(points) - 2) * spacing + spacing / 2
    return spline((np.asarray(voxels)[:, None] + 0.5 - centre[None, :]) / spacing)


def halves(matrix):
    matrix = np.asarray(matrix, np.float32)
    high = matrix.astype(bf16)
    return high, (matrix - high.astype(np.float32)).astype(bf16)


def split(values):
    high = values.astype(bf16)
    return high, (values - high.astype(f32)).astype(bf16)


def mm(a, b):
    return jnp.dot(a, b, preferred_element_type=f32)


def mm3(values, high, low):
    a, b = split(values)
    return mm(a, high) + mm(b, high) + mm(a, low)


def lanes(shape):
    return lax.broadcasted_iota(jnp.int32, shape, len(shape) - 1)


def rows_of(shape):
    return lax.broadcasted_iota(jnp.int32, shape, len(shape) - 2)


def rolled(values, shift):
    shift %= values.shape[-1]
    return values if shift == 0 else pltpu.roll(values, shift, values.ndim - 1)


def within(mib):
    return pltpu.CompilerParams(vmem_limit_bytes=mib * 2**20)


def whole(n):
    return [pl.BlockSpec(memory_space=VMEM)] * n


PARTS = ((0, 4), (4, 12), (16, 16), (32, 16), (48, 16))


def faces_kernel(w_hbm, f_hbm, xf_ref, xo_ref, yf_ref, yo_ref, zf_ref, zo_ref, s_ref, t_ref, d_ref, w_ref, f_ref, sem):
    def copies(g):
        part = pl.ds(*PARTS[g])
        return [
            pltpu.make_async_copy(hbm.at[part], ref.at[part], sem.at[i, g])
            for i, (hbm, ref) in enumerate(((w_hbm, w_ref), (f_hbm, f_ref)))
        ]

    for g in range(len(PARTS)):
        for copy in copies(g):
            copy.start()
    lane = lanes((64, 128))
    for ref in (s_ref, t_ref):
        ref[:, 0:8, :] = jnp.zeros((68, 8, 128), f32)
        ref[:, 72:80, :] = jnp.zeros((68, 8, 128), f32)
        for x in (0, 1, 66, 67):
            ref[x, 8:72, :] = jnp.zeros((64, 128), f32)

    for g, (start, size) in enumerate(PARTS):
        for copy in copies(g):
            copy.wait()
        for x in range(start, start + size):
            w = w_ref[x]
            f = f_ref[x]
            s = w + f
            d = w - f
            s_ref[x + 2, 8:72, :] = s
            t_ref[x + 2, 8:72, :] = 8.0 * s
            d_ref[x] = d
            for j in range(2):
                yf_ref[j, x : x + 1, :] = s[62 + j : 63 + j]
                yf_ref[2 + j, x : x + 1, :] = d[62 + j : 63 + j]
                yo_ref[j, x : x + 1, :] = s[j : j + 1]
                yo_ref[2 + j, x : x + 1, :] = d[j : j + 1]
            i = x % 32
            here = (lane >= 4 * i) & (lane < 4 * i + 4)
            packed_s = rolled(s, 4 * i + 2) if i == 0 else jnp.where(here, rolled(s, 4 * i + 2), packed_s)
            packed_d = rolled(d, 4 * i + 2) if i == 0 else jnp.where(here, rolled(d, 4 * i + 2), packed_d)
            if i == 31:
                zo_ref[x // 32] = packed_s
                zo_ref[2 + x // 32] = packed_d

    for j in range(2):
        xf_ref[j] = s_ref[64 + j, 8:72, :]
        xf_ref[2 + j] = d_ref[62 + j]
        xo_ref[j] = s_ref[2 + j, 8:72, :]
        xo_ref[2 + j] = d_ref[j]
        zf_ref[j] = jnp.where(lane % 4 < 2, zo_ref[2 * j], rolled(zo_ref[2 * j + 1], 2))


def faces(w, f):
    shapes = [(4, 64, 128)] * 4 + [(2, 64, 128), (4, 64, 128)] + [(68, 80, 128)] * 2 + [(64, 64, 128)]
    return pl.pallas_call(
        faces_kernel,
        in_specs=[pl.BlockSpec(memory_space=pltpu.HBM)] * 2,
        out_specs=whole(9),
        out_shape=[jax.ShapeDtypeStruct(s, f32) for s in shapes],
        scratch_shapes=[
            VMEM((64, 64, 128), f32),
            VMEM((64, 64, 128), f32),
            pltpu.SemaphoreType.DMA((2, len(PARTS))),
        ],
        compiler_params=within(16),
        name="faces",
    )(*(pltpu.with_memory_space_constraint(v, pltpu.HBM) for v in (w, f)))


def bend_kernel(sizes, c_ref, k_ref, bf_ref, bk_ref, u_ref, k2_ref):
    nx, ny, nz = sizes
    ix, iy, iz = (lax.axis_index(n) for n in ("gx", "gy", "gz"))
    u_ref[...] = jnp.zeros_like(u_ref)
    for a in range(3):
        for p in range(8):
            at = 20 * (p + 2) + 2
            u_ref[a * 16 + 2 : a * 16 + 10, at : at + 16] = c_ref[a, p]
    lane = lanes((48, 256))
    row = rows_of((48, 256)) % 16
    gp = lane // 20 - 2 + 8 * ix
    gr = lane % 20 - 2 + 16 * iz
    gq = row - 2 + 8 * iy
    inside = (gp >= 0) & (gp < 8 * nx) & (gq >= 0) & (gq < 8 * ny) & (gr >= 0) & (gr < 16 * nz)

    def around(u, step):
        total = pltpu.roll(u, 1, 0) + pltpu.roll(u, u.shape[0] - 1, 0)
        for shift in (1, -1, step, -step):
            total = total + rolled(u, shift)
        return total - 6.0 * u

    u = around(u_ref[...], 20)
    u = around(jnp.where(inside, u, 0.0), 20) * BEND
    keep = lanes((48, 128)) < 120
    bf_ref[:, 0:128] = jnp.where(keep, u[:, 0:128], 0.0)
    bf_ref[:, 128:256] = jnp.where(keep, pltpu.roll(u, 136, 1)[:, 0:128], 0.0)

    kx, ky, kz = 2 * nx, 2 * ny, 4 * nz
    k2_ref[...] = jnp.zeros_like(k2_ref)
    parts = []
    for a in range(3):
        total = None
        for p in range(6):
            i = 6 * a + p
            k2_ref[i, 0:ky, 0:kz] = k_ref[a, jnp.clip(2 * ix - 2 + p, 0, kx - 1)]
            tile = pltpu.roll(k2_ref[i], (18 - 2 * iy) % 16, 0)[0:8]
            tile = pltpu.roll(tile, (130 - 4 * iz + 8 * p) % 128, 1)
            total = tile if p == 0 else jnp.where(lanes((8, 128)) // 8 == p, tile, total)
        parts.append(total)
    lane = lanes((24, 128))
    row = rows_of((24, 128)) % 8
    gp, gq, gr = 2 * ix - 2 + lane // 8, 2 * iy - 2 + row, 4 * iz - 2 + lane % 8
    inside = (gp >= 0) & (gp < kx) & (gq >= 0) & (gq < ky) & (gr >= 0) & (gr < kz) & (lane < 48)
    u = jnp.where(inside, jnp.concatenate(parts, 0), 0.0)
    u = around(jnp.where(inside, around(u, 8), 0.0), 8) * BEND
    own = (lane // 16 == 1) & (row // 2 == 1) & ((lane % 8 + 2) // 4 == 1)
    bk_ref[...] = rolled(jnp.where(own, u, 0.0), 80)


def bend(sizes, control, coarse):
    return pl.pallas_call(
        functools.partial(bend_kernel, sizes),
        in_specs=whole(2),
        out_specs=whole(2),
        out_shape=[
            jax.ShapeDtypeStruct((48, 256), f32),
            jax.ShapeDtypeStruct((24, 128), f32),
        ],
        scratch_shapes=[VMEM((48, 256), f32), VMEM((18, 16, 128), f32)],
        cost_estimate=pl.CostEstimate(flops=4000000, bytes_accessed=1000000, transcendentals=0),
        compiler_params=within(8),
        name="bend",
    )(control, coarse)


@functools.cache
def tables():
    own = np.arange(64)
    cross = np.arange(-2, 2)
    wy = np.zeros((24, 64))
    wy[0:12] = weights(own, 12, SPF).T
    wy[16:22] = weights(own, 6, SPC).T
    high, low = halves(wy)
    left = np.concatenate(
        [np.concatenate([high, high], 1), np.concatenate([low, np.zeros_like(low)], 1)], 0
    )
    wc = np.zeros((8, 8, 128), np.float32)
    for j in range(4):
        wc[j, :, :] = weights(cross, 12, SPF)[j, 0:8, None]
        wc[4 + j, 0:6, :] = weights(cross, 6, SPC)[j, :, None]
    fine_scale = SPF**-1.5 / 24.0
    coarse_scale = SPC**-1.5 / 24.0
    wz = np.zeros((2, 128, 128))
    wz[0, :, 0:20] = weights(np.arange(128), 20, SPF) * fine_scale
    wz[1, :, 0:8] = weights(np.arange(128), 8, SPC) * coarse_scale
    wz_high, wz_low = halves(wz)
    m = np.zeros((4, 128, 384))
    fx, cx = weights(own, 12, SPF), weights(own, 6, SPC)
    fz = weights(cross, 20, SPF) * fine_scale
    cz = weights(cross, 8, SPC) * coarse_scale
    fz = np.concatenate([fz, weights(np.arange(126, 128), 20, SPF) * fine_scale])
    cz = np.concatenate([cz, weights(np.arange(126, 128), 8, SPC) * coarse_scale])
    for x in range(64):
        for j in range(6):
            line = m[x // 32 + 2 * (j // 4), 4 * (x % 32) + j % 4]
            for p in range(12):
                at = 128 * (p // 6) + 20 * (p % 6)
                line[at : at + 20] = fx[x, p] * fz[j]
            for p in range(6):
                at = 256 + 80 + 8 * p
                line[at : at + 8] = cx[x, p] * cz[j]
    m_high, m_low = halves(m)
    return left, wc, wz_high, wz_low, m_high, m_low


def along(left, force):
    high, low = split(force)
    both = mm(left, jnp.concatenate([high, low], 0))
    return both[0:24] + both[24:48]


def interior_kernel(s_ref, t_ref, d_ref, left_ref, af_ref, ac_ref, tf_ref, tc_ref):
    fx = weights(np.arange(8), 5, SPF)
    cx = weights(np.arange(64), 6, SPC)
    left = left_ref[...]

    def force(x):
        d = d_ref[x]
        f0 = (s_ref[x, 8:72, :] - s_ref[x + 4, 8:72, :]) + (t_ref[x + 3, 8:72, :] - t_ref[x + 1, 8:72, :])
        s, t = s_ref.at[x + 2], t_ref.at[x + 2]
        f1 = (s[6:70, :] - s[10:74, :]) + (t[9:73, :] - t[7:71, :])
        s, t = s[8:72, :], t[8:72, :]
        f2 = (rolled(s, 2) - rolled(s, 126)) + (rolled(t, 127) - rolled(t, 1))
        return [f0 * d, f1 * d, f2 * d]

    def layers(b):
        for i in range(0, 8, 2):
            section = along(left, jnp.concatenate(force(8 * b + i) + force(8 * b + i + 1), 1))
            for k in range(6):
                at, a = 8 * b + i + k // 3, k % 3
                cols = slice(128 * k, 128 * k + 128)
                tf_ref[at, 16 * a : 16 * a + 16, :] = section[0:16, cols]
                tc_ref[at, 8 * a : 8 * a + 8, :] = section[16:24, cols]

    def block(b):
        for k in range(5):
            total = af_ref[b + k]
            for r in range(8):
                weight = float(fx[r, k])
                if weight != 0.0:
                    total = total + weight * tf_ref[8 * b + r]
            af_ref[b + k] = total
        for k in range((b + 2) // 4, (b + 2) // 4 + 4):
            total = ac_ref[k]
            for r in range(8):
                total = total + float(cx[8 * b + r, k]) * tc_ref[8 * b + r]
            ac_ref[k] = total

    af_ref[...] = jnp.zeros_like(af_ref)
    ac_ref[...] = jnp.zeros_like(ac_ref)
    for b in range(8):
        layers(b)
        if b > 0:
            block(b - 1)
    block(7)


def interior(s, s8, d):
    left = tables()[0]
    return pl.pallas_call(
        interior_kernel,
        in_specs=whole(4),
        out_specs=whole(2),
        out_shape=[
            jax.ShapeDtypeStruct((12, 48, 128), f32),
            jax.ShapeDtypeStruct((6, 24, 128), f32),
        ],
        scratch_shapes=[VMEM((64, 48, 128), f32), VMEM((64, 24, 128), f32)],
        cost_estimate=pl.CostEstimate(flops=40000000, bytes_accessed=4000000, transcendentals=0),
        compiler_params=within(16),
        name="interior",
    )(s, s8, d, jnp.asarray(left))


def crossing(first, second):
    sm2, sm1, dm2, dm1 = (first[i] for i in range(4))
    s0, s1, d0, d1 = (second[i] for i in range(4))
    return [-s0 * dm2, (8.0 * s0 - s1) * dm1, (sm2 - 8.0 * sm1) * d0, sm1 * d1]


def finish_kernel(
    af_ref, ac_ref, xr_ref, xo_ref, yr_ref, yo_ref, zr_ref, zo_ref, bf_ref, bk_ref, left_ref, wc_ref, wzh_ref, wzl_ref, mh_ref, ml_ref,
    chunk_ref, fine_ref, sf_ref, sc_ref,
):
    n = chunk_ref.shape[0]
    edge_f = weights(np.arange(-2, 2), 4, SPF)
    edge_c = weights(np.arange(-2, 2), 4, SPC)
    left = left_ref[...]
    lane = lanes((64, 128))

    edge = along(left, jnp.concatenate(crossing(xr_ref, xo_ref), 1))
    sf_ref[...] = af_ref[...]
    sc_ref[...] = ac_ref[...]
    for k in range(4):
        for j in range(4):
            cols = slice(128 * j, 128 * j + 128)
            fine = float(edge_f[j, k]) * edge[0:16, cols]
            coarse = float(edge_c[j, k]) * edge[16:24, cols]
            total_f = fine if j == 0 else total_f + fine
            total_c = coarse if j == 0 else total_c + coarse
        sf_ref[k, 0:16, :] += total_f
        sc_ref[k, 0:8, :] += total_c

    edge = along(left, jnp.concatenate(crossing(yr_ref, yo_ref), 1))
    for p in range(12):
        total = sf_ref[p, 16:24, :]
        for j in range(4):
            total = total + wc_ref[j] * edge[p : p + 1, 128 * j : 128 * j + 128]
        sf_ref[p, 16:24, :] = total
    for p in range(6):
        total = sc_ref[p, 8:16, :]
        for j in range(4):
            total = total + wc_ref[4 + j] * edge[16 + p : 17 + p, 128 * j : 128 * j + 128]
        sc_ref[p, 8:16, :] = total

    zf = mm3(sf_ref[...].reshape(576, 128), wzh_ref[0], wzl_ref[0])
    zc = mm3(sc_ref[...].reshape(144, 128), wzh_ref[1], wzl_ref[1])
    fine = []
    for h in range(2):
        total = zf[288 * h : 288 * h + 48]
        for i in range(1, 6):
            total = total + rolled(zf[48 * (6 * h + i) : 48 * (6 * h + i) + 48], 20 * i)
        fine.append(total + bf_ref[:, 128 * h : 128 * h + 128])
    coarse = bk_ref[...] + rolled(zc[0:24], 80)
    for p in range(1, 6):
        coarse = coarse + rolled(zc[24 * p : 24 * p + 24], 80 + 8 * p)

    j = lane % 4
    extra = None
    for h in range(2):
        s = jnp.where(j < 2, rolled(zr_ref[0], -2 * h) - zo_ref[h], zo_ref[h])
        d = jnp.where(j < 2, rolled(zr_ref[1], -2 * h), zo_ref[2 + h])
        slope = jnp.where(j >= 2, rolled(s, 2), 0.0) - jnp.where(j < 2, rolled(s, 126), 0.0)
        slope = slope + 8.0 * (
            jnp.where(j == 1, rolled(s, 127), 0.0) - jnp.where(j == 2, rolled(s, 1), 0.0)
        )
        wrapped = jnp.where(j < 2, -slope * zo_ref[2 + h], 0.0)
        part = along(left, jnp.concatenate([slope * d, wrapped], 1))
        part = mm3(part[:, 0:128], mh_ref[h], ml_ref[h]) + mm3(part[:, 128:256], mh_ref[2 + h], ml_ref[2 + h])
        extra = part if extra is None else extra + part

    zero8 = jnp.zeros((8, 128), f32)
    zero32 = jnp.zeros((32, 128), f32)
    low = fine[0] + jnp.concatenate([zero32, extra[0:16, 0:128]], 0)
    high = fine[1] + jnp.concatenate([zero32, extra[0:16, 128:256]], 0)
    spread = jnp.concatenate(
        [coarse[0:8], zero8, coarse[8:16], zero8, coarse[16:24] + extra[16:24, 256:384], zero8], 0
    )
    fine_ref[:, 0:128] = low
    fine_ref[:, 128:256] = high
    lane = lanes((48, 128))
    chunk = jnp.where(lane < 40, low, jnp.where(lane < 80, rolled(high, 88), spread))
    last = chunk[40:44]
    beside = (lanes((4, 128)) >= 80) & (lanes((4, 128)) < 120)
    for i in range(n):
        for a in range(3):
            size = 8 if a == 2 else 12
            chunk_ref[i, 12 * a : 12 * a + size, :] = chunk[16 * a : 16 * a + size]
        chunk_ref[i, 6:10, :] = jnp.where(beside, rolled(last, 80), chunk[6:10])
        chunk_ref[i, 18:22, :] = jnp.where(beside, rolled(last, 40), chunk[22:26])


def finish(n, *values):
    constants = tables()
    return pl.pallas_call(
        finish_kernel,
        in_specs=whole(16),
        out_specs=whole(2),
        out_shape=[
            jax.ShapeDtypeStruct((n, 32, 128), f32),
            jax.ShapeDtypeStruct((48, 256), f32),
        ],
        scratch_shapes=[VMEM((12, 48, 128), f32), VMEM((6, 24, 128), f32)],
        compiler_params=within(12),
        name="finish",
    )(*values, *(jnp.asarray(c) for c in constants))


def sides(ref, axis):
    n = ref.shape[0]
    i = lax.axis_index(axis)
    return ref[jnp.maximum(i - 1, 0)], i > 0, ref[jnp.minimum(i + 1, n - 1)], i < n - 1


def x_kernel(ny, got_ref, fine_ref, chunk_ref, own_ref, pack_ref):
    n = got_ref.shape[0]
    lane = lanes((24, 128))
    coarse = jnp.zeros((24, 128), f32)
    for j in range(n):
        part = jnp.concatenate([got_ref[j, 12 * a : 12 * a + 8, :] for a in range(3)], 0)
        first, last = max(0, 16 * j - 16), min(16 * n, 16 * j + 32)
        here = (lane >= first) & (lane < last) & (rows_of((24, 128)) % 8 < 6)
        coarse = coarse + jnp.where(here, rolled(part, 16 * j - 96), 0.0)
    low, has_low, high, has_high = sides(got_ref, "gx")
    lane = lanes((12, 128))
    middle = (lane >= 40) & (lane < 80)
    own_ref[...] = fine_ref[...]
    for a in range(3):
        size = 8 if a == 2 else 12
        rows, there = slice(16 * a, 16 * a + size), slice(12 * a, 12 * a + size)
        keep = middle[0:size]
        own_ref[rows, 0:128] += jnp.where(keep & has_low, low[there], 0.0)
        own_ref[rows, 128:256] += jnp.where(keep & has_high, rolled(high[there], 40), 0.0)
    keep = middle[0:4]
    own_ref[40:44, 0:128] += jnp.where(keep & has_low, rolled(low[18:22], -40), 0.0)
    own_ref[40:44, 128:256] += jnp.where(keep & has_high, rolled(high[6:10], -40), 0.0)
    pack_ref[0:24, :] = coarse
    lane = lanes((2, 128))
    for m, q in ((0, 0), (2, 10)):
        last = jnp.zeros((2, 128), f32)
        for a in range(3):
            first = own_ref[16 * a + q : 16 * a + q + 2, 0:128]
            second = own_ref[16 * a + q : 16 * a + q + 2, 128:256]
            pack_ref[24 + 4 * a + m : 26 + 4 * a + m, :] = jnp.where(lane < 40, second, first)
            last = jnp.where((lane >= 40 * a) & (lane < 40 * a + 40), rolled(second, 40 * a - 40), last)
        pack_ref[36 + m : 38 + m, :] = last
    for i in range(ny):
        chunk_ref[i] = pack_ref[...]


def x_stage(ny, got, fine):
    return pl.pallas_call(
        functools.partial(x_kernel, ny),
        in_specs=whole(2),
        out_specs=whole(2),
        out_shape=[
            jax.ShapeDtypeStruct((ny, 40, 128), f32),
            jax.ShapeDtypeStruct((48, 256), f32),
        ],
        scratch_shapes=[VMEM((40, 128), f32)],
        compiler_params=within(4),
        name="xstage",
    )(got, fine)


def lane_of(p):
    return 128 * (p // 6), 20 * (p % 6)


def y_kernel(nz, got_ref, fine_ref, chunk_ref, own_ref, sum_ref):
    n = got_ref.shape[0]
    sum_ref[...] = jnp.zeros_like(sum_ref)
    for j in range(n):
        for a in range(3):
            at = 24 * a + 2 * j
            sum_ref[at : at + 6, :] += got_ref[j, 8 * a : 8 * a + 6, :]
    low, has_low, high, has_high = sides(got_ref, "gy")
    own_ref[...] = fine_ref[...]
    lane = lanes((2, 128))
    inner, tail = lane < 40, (lane >= 40) & (lane < 80)
    for a in range(3):
        for got, valid, m, q in ((low, has_low, 2, 2), (high, has_high, 0, 8)):
            rows = slice(16 * a + q, 16 * a + q + 2)
            first = got[24 + 4 * a + m : 26 + 4 * a + m]
            last = rolled(got[36 + m : 38 + m], 40 - 40 * a)
            second = jnp.where(inner, first, jnp.where(tail, last, 0.0))
            own_ref[rows, 0:128] += jnp.where(valid & ~inner, first, 0.0)
            own_ref[rows, 128:256] += jnp.where(valid, second, 0.0)
    lane = lanes((8, 128))
    border = jnp.zeros((8, 128), f32)
    for a in range(3):
        for p in range(8):
            tile, base = lane_of(p + 2)
            v = own_ref[16 * a + 2 : 16 * a + 10, tile : tile + 128]
            at = 32 * a + 4 * p
            border = jnp.where((lane >= at) & (lane < at + 2), rolled(v, at - base), border)
            border = jnp.where((lane >= at + 2) & (lane < at + 4), rolled(v, at - base - 16), border)
    for i in range(nz):
        for a in range(3):
            chunk_ref[i, 16 * a : 16 * a + 16, :] = sum_ref[24 * a + 2 : 24 * a + 18, :]
        chunk_ref[i, 48:56, :] = border


def y_stage(nz, got, fine):
    return pl.pallas_call(
        functools.partial(y_kernel, nz),
        in_specs=whole(2),
        out_specs=whole(2),
        out_shape=[
            jax.ShapeDtypeStruct((nz, 56, 128), f32),
            jax.ShapeDtypeStruct((48, 256), f32),
        ],
        scratch_shapes=[VMEM((72, 128), f32)],
        compiler_params=within(4),
        name="ystage",
    )(got, fine)


def z_kernel(nx, ny, got_ref, fine_ref, out_fine_ref, out_coarse_ref):
    n = got_ref.shape[0]
    low, has_low, high, has_high = sides(got_ref, "gz")
    low = jnp.where(has_low, low[48:56], 0.0)
    high = jnp.where(has_high, high[48:56], 0.0)
    lane = lanes((8, 128))
    for a in range(3):
        for p in range(8):
            tile, base = lane_of(p + 2)
            v = fine_ref[16 * a + 2 : 16 * a + 10, tile : tile + 128]
            at = 32 * a + 4 * p
            v = v + jnp.where((lane >= base + 2) & (lane < base + 4), rolled(low, base - at), 0.0)
            v = v + jnp.where((lane >= base + 16) & (lane < base + 18), rolled(high, base + 16 - at), 0.0)
            out_fine_ref[a, p] = rolled(v, -(base + 2))[:, 0:16]

    lane = lanes((48, 128))
    k = lane % 8
    parts = [got_ref[m, 0:48, :] for m in range(n)]
    tiles = []
    for m in range(0, n, 2):
        total = jnp.where(k < 6, rolled(parts[m], -2), 0.0) + jnp.where(k >= 2, rolled(parts[m + 1], 2), 0.0)
        if m > 0:
            total = total + jnp.where(k < 2, rolled(parts[m - 1], -6), 0.0)
        if m + 2 < n:
            total = total + jnp.where(k >= 6, rolled(parts[m + 2], 6), 0.0)
        tiles.append(total)
    per = len(tiles)
    slot = lane // 8 % per
    for h in range(per):
        total = rolled(tiles[0], -8 * h)
        for m in range(1, per):
            total = jnp.where(slot == m, rolled(tiles[m], 8 * (m - h)), total)
        for g in range(2 * nx // per):
            points = rolled(total, -8 * per * g)
            for a in range(3):
                out_coarse_ref[a, per * g + h] = points[16 * a : 16 * a + 2 * ny, 0 : 4 * n]


def z_stage(sizes, got, fine):
    nx, ny, nz = sizes
    return pl.pallas_call(
        functools.partial(z_kernel, nx, ny),
        in_specs=whole(2),
        out_specs=whole(2),
        out_shape=[
            jax.ShapeDtypeStruct((3, 8, 8, 16), f32),
            jax.ShapeDtypeStruct((3, 2 * nx, 2 * ny, 4 * nz), f32),
        ],
        compiler_params=within(6),
        name="zstage",
    )(got, fine)


def shifted_up(values, axis):
    return lax.ppermute(values, axis, [(i, i + 1) for i in range(lax.axis_size(axis) - 1)])


def exchanged(chunks, axis):
    return lax.all_to_all(chunks, axis, split_axis=0, concat_axis=0, tiled=True)


def per_device(warped_image, fixed_image, fine_control, coarse_control):
    sizes = tuple(lax.axis_size(n) for n in ("gx", "gy", "gz"))
    xf, xo, yf, yo, zf, zo, s, s8, d = faces(warped_image, fixed_image)
    yr = shifted_up(yf, "gy")
    zr = shifted_up(zf, "gz")
    xr = shifted_up(xf, "gx")
    bent_fine, bent_coarse = bend(sizes, fine_control, coarse_control)
    fine, coarse = interior(s, s8, d)
    chunk, fine = finish(sizes[0], fine, coarse, xr, xo, yr, yo, zr, zo, bent_fine, bent_coarse)
    chunk, fine = x_stage(sizes[1], exchanged(chunk, "gx"), fine)
    chunk, fine = y_stage(sizes[2], exchanged(chunk, "gy"), fine)
    return tuple(z_stage(sizes, exchanged(chunk, "gz"), fine))


def solution(mesh):
    in_specs = (P("gx", "gy", "gz"), P("gx", "gy", "gz"), P(None, "gx", "gy", "gz"), P())
    out_specs = (P(None, "gx", "gy", "gz"), P())
    return jax.shard_map(
        per_device, mesh=mesh, in_specs=in_specs, out_specs=out_specs, check_vma=False
    )
```
